32 devices in a mesh: rep: 2 (over x), dp: 16 (over y, z, core).
Axes of the slice: x: 2, y: 2, z: 4, core: 2. Of those that a mesh axis runs over, the one named last changes fastest.
Arguments:
- g_w_gate: bfloat16 [32, 2, 1024, 3584], P(('rep', 'dp')), parts along dimension 0
- g_w_up: bfloat16 [32, 2, 1024, 3584], P(('rep', 'dp')), parts along dimension 0
- g_w_down: bfloat16 [32, 2, 3584, 1024], P(('rep', 'dp')), parts along dimension 0
- w_gate: bfloat16 [2, 1024, 3584], replicated
- w_up: bfloat16 [2, 1024, 3584], replicated
- w_down: bfloat16 [2, 3584, 1024], replicated
- m_w_gate: float32 [2, 1024, 3584], P(None, 'dp')
- m_w_up: float32 [2, 1024, 3584], P(None, 'dp')
- m_w_down: float32 [2, 3584, 1024], P(None, 'dp')
- v_w_gate: float32 [2, 1024, 3584], P(None, 'dp')
- v_w_up: float32 [2, 1024, 3584], P(None, 'dp')
- v_w_down: float32 [2, 3584, 1024], P(None, 'dp')
Outputs:
- output 1: bfloat16 [4, 1024, 3584], P('rep'), parts along dimension 0
- output 2: bfloat16 [4, 1024, 3584], P('rep'), parts along dimension 0
- output 3: bfloat16 [4, 3584, 1024], P('rep'), parts along dimension 0
- output 4: float32 [4, 1024, 3584], P('rep', 'dp'), parts along dimension 0
- output 5: float32 [4, 1024, 3584], P('rep', 'dp'), parts along dimension 0
- output 6: float32 [4, 3584, 1024], P('rep', 'dp'), parts along dimension 0
- output 7: float32 [4, 1024, 3584], P('rep', 'dp'), parts along dimension 0
- output 8: float32 [4, 1024, 3584], P('rep', 'dp'), parts along dimension 0
- output 9: float32 [4, 3584, 1024], P('rep', 'dp'), parts along dimension 0
There are 2 independent parts. The reference program is written for one: setup_inputs(seed, part) draws one part's arguments, and reference() takes and returns one part's arrays. A program takes and returns all parts, laid end to end along the dimension named above; an argument that names none is the same for every part.
All inputs are finite; a program needn't handle non-finite values.
Results may differ from the reference program's by a relative error of at most 0.022.
Values are sent between devices in bfloat16 or wider.
A program may use at most 2 GiB of HBM per device.

```python
import jax
import jax.numpy as jnp
from jax import lax

DEVICES = 16
D = 1024
FF = 3584
LAYERS = 2
NAMES = ("w_gate", "w_up", "w_down")
SHAPES = {"w_gate": (LAYERS, D, FF), "w_up": (LAYERS, D, FF), "w_down": (LAYERS, FF, D)}


def setup_inputs(seed: int = 0, part: int = 0) -> dict:
    kz, *keys = jax.random.split(jax.random.key(seed), 1 + 5 * len(NAMES))
    loud = 2.0 ** jax.random.uniform(kz, (), jnp.float32, -1.0, 1.0)
    drawn = {}
    for name, key, both in zip(NAMES, keys[:3], keys[3:6], strict=True):
        own = jax.random.normal(jax.random.fold_in(key, part), (DEVICES, *SHAPES[name]), jnp.float32)
        shared = jax.random.normal(jax.random.fold_in(both, part), SHAPES[name], jnp.float32)
        drawn["g_" + name] = (loud * (0.7 * shared / DEVICES + 0.7 * own * DEVICES**-0.5)).astype(jnp.bfloat16)
    for name, key in zip(NAMES, keys[6:9], strict=True):
        drawn[name] = (jax.random.normal(key, SHAPES[name], jnp.float32) * SHAPES[name][1] ** -0.5).astype(jnp.bfloat16)
    for name, key in zip(NAMES, keys[9:12], strict=True):
        drawn["m_" + name] = loud * 0.5 * jax.random.normal(key, SHAPES[name], jnp.float32)
    for name, key in zip(NAMES, keys[12:15], strict=True):
        drawn["v_" + name] = loud * loud * jax.random.uniform(key, SHAPES[name], jnp.float32, 0.5, 1.5)
    return drawn


def adamw(w, m, v, g):
    m = 0.9 * m + 0.1 * g
    v = 0.95 * v + 0.05 * g * g
    step = m * lax.rsqrt(v + 1e-8) + 0.1 * w
    return (w - 0.02 * step).astype(jnp.bfloat16), m, v


def reference(g_w_gate, g_w_up, g_w_down, w_gate, w_up, w_down, m_w_gate, m_w_up, m_w_down, v_w_gate, v_w_up, v_w_down):
    def total(terms):
        return lax.scan(lambda so_far, term: (so_far + term.astype(jnp.float32), None), jnp.zeros(terms.shape[1:], jnp.float32), terms)[0]

    gradients = [total(terms).astype(jnp.bfloat16).astype(jnp.float32) for terms in (g_w_gate, g_w_up, g_w_down)]
    new = [
        adamw(w.astype(jnp.float32), m, v, g)
        for w, m, v, g in zip((w_gate, w_up, w_down), (m_w_gate, m_w_up, m_w_down), (v_w_gate, v_w_up, v_w_down), gradients, strict=True)
    ]
    return tuple(one[which] for which in range(3) for one in new)
```

```python
import functools

import jax
import jax.numpy as jnp
from jax import lax
from jax.experimental import pallas as pl
from jax.experimental.pallas import tpu as pltpu
from jax.sharding import PartitionSpec as P

MESH = pl.DeviceIdType.MESH
ANY = pl.BlockSpec(memory_space=pl.ANY)
ROUNDS = 8
SLOTS = 4
LOADS = 2
NAMES = ("gate", "up", "down")
TYPES = (("y",) * 8, ("z",) * 8, ("y", "y", "y", "z") * 2)
LAGS = {
    "y": (("fetch", 0), ("moments", 4), ("first", 3), ("near", 4), ("far", 5), ("step", 6), ("pass1", 7), ("pass2", 8), ("pass3", 9)),
    "z": (("fetch", 0), ("moments", 5), ("first", 3), ("near", 4), ("far", 5), ("cross", 6), ("step", 7), ("pass0", 8), ("pass1", 9), ("pass2", 10)),
}
ORDER = ("fetch", "moments", "first", "near", "far", "cross", "step", "pass0", "pass1", "pass2", "pass3")
KEYS = ("s", "d", "rb", "wb", "gb", "wl", "ml", "vl", "ld", "dr", "ds", "ss", "rr", "ar", "ad", "ay", "az", "lo", "adr", "mo", "free")


def new_moments(m, v, g):
    return 0.9 * m + 0.1 * g, 0.95 * v + 0.05 * g * g


def new_weight(w, m, v):
    return (w - 0.02 * (m * lax.rsqrt(v + 1e-8) + 0.1 * w)).astype(jnp.bfloat16)


def piece(which, r):
    layer, q = r // 4, lax.rem(r, 4)
    if which == 2:
        return layer, pl.ds(pl.multiple_of(q // 2 * 112, 112), 112), pl.ds(pl.multiple_of(lax.rem(q, 2) * 512, 512), 512)
    return layer, pl.ds(pl.multiple_of(q * 16, 16), 16), pl.ds(0, 3584)


def shape_of(which):
    return (112, 512) if which == 2 else (16, 3584)


def scratch(which):
    rows, cols = shape_of(which)
    bf, f32, dma = jnp.bfloat16, jnp.float32, pltpu.SemaphoreType.DMA
    return (
        pltpu.VMEM((SLOTS, 8, rows, cols), bf),
        pltpu.VMEM((SLOTS, 8, rows, cols), bf),
        pltpu.VMEM((ROUNDS, 9 if which == 0 else 11, rows, cols), bf),
        pltpu.VMEM((ROUNDS, rows, cols), bf),
        pltpu.VMEM((ROUNDS, rows, cols), bf),
        pltpu.VMEM((LOADS, rows, cols), bf),
        pltpu.VMEM((LOADS, rows, cols), f32),
        pltpu.VMEM((LOADS, rows, cols), f32),
        dma((SLOTS,)),
        dma((SLOTS,)),
        dma,
        dma((SLOTS,)),
        dma((ROUNDS, 11)),
        dma((ROUNDS, 8)),
        dma,
        dma((2,)),
        dma((2,)),
        dma,
        dma,
        dma((LOADS, 3)),
        pltpu.SemaphoreType.REGULAR,
    )


class Weight:
    pass


def kernel(*refs):
    rep, me = lax.axis_index("rep"), lax.axis_index("dp")
    y, z, c = me // 8, lax.rem(me // 2, 4), lax.rem(me, 2)
    own = me // 2
    partner, across = me + 1 - 2 * c, me + 8 - 16 * y
    mid = (z > 0) & (z < 3)
    corner = (z == 0) | (z == 3)
    low = 1 - z // 2
    odd = lax.rem(z, 2)
    onward = me + 4 * low - 2
    e = (3 * low, 1 + low, low * (1 - z) + (1 - low) * (5 - z))
    e_to = (onward, onward, me + 2 - 4 * odd)
    e_slot = (e[0], e[1] + z // 2 * (1 - odd) * (4 - e[1]), e[2] + odd * (4 - e[2]))
    f = (z + 1 - 2 * odd, 2 - z // 2, 3 * low)
    f_to = (onward, me + 2 - 4 * low, me + 2 - 4 * low)

    inputs, outputs, rest = refs[:12], refs[12:18], refs[18:]
    weights = []
    for i in range(3):
        x = Weight()
        x.which, x.types = i, TYPES[i]
        x.g, x.w, x.m, x.v = inputs[i], inputs[3 + i], inputs[6 + i], inputs[9 + i]
        x.out, x.gout = outputs[i], outputs[3 + i]
        for key, ref in zip(KEYS, rest[i * len(KEYS) : (i + 1) * len(KEYS)], strict=True):
            setattr(x, key, ref)
        weights.append(x)

    def send(src, dst, sent, got, to):
        return pltpu.make_async_remote_copy(src_ref=src, dst_ref=dst, send_sem=sent, recv_sem=got, device_id=(rep, to), device_id_type=MESH)

    def arrive(ref, sem):
        send(ref, ref, sem, sem, partner).wait_recv()

    def left(ref, sem):
        send(ref, ref, sem, sem, partner).wait_send()

    def blocks(x, ref, r, j, core):
        layer, rows, cols = piece(x.which, r)
        return ref.at[layer, j, core, rows, cols]

    def mine(x, ref, r):
        layer, rows, cols = piece(x.which, r)
        return ref.at[layer, rows, cols]

    def add(x, dst, *terms):
        def slab(k, carry):
            rows = pl.ds(pl.multiple_of(k * 16, 16), 16)
            total = terms[0][rows, :].astype(jnp.float32)
            for term in terms[1:]:
                total += term[rows, :].astype(jnp.float32)
            dst[rows, :] = total.astype(jnp.bfloat16)
            return carry

        lax.fori_loop(0, shape_of(x.which)[0] // 16, slab, 0)

    def ends(x, r, base):
        def when(then):
            @pl.when(mid)
            def _():
                arrive(x.rb.at[r, base + z], x.rr.at[r, base + z])
                arrive(x.rb.at[r, base + 4], x.rr.at[r, base + 4])
                then(x.rb.at[r, base + z], x.rb.at[r, base + 4])

            @pl.when(corner)
            def _():
                at = base + 4 - z // 3
                arrive(x.rb.at[r, at], x.rr.at[r, at])
                then(x.rb.at[r, at])

        return when

    def fetch(x, kind, r):
        slot = lax.rem(r, SLOTS)

        @pl.when(r >= SLOTS)
        def _():
            left(x.s.at[slot, pl.ds(0, 7)], x.ss.at[slot])
            pl.semaphore_wait(x.free, 1)

        pltpu.make_async_copy(blocks(x, x.g, r, slice(None), c), x.s.at[slot], x.ld.at[slot]).start()
        send(blocks(x, x.g, r, slice(None), 1 - c), x.d.at[slot], x.ds, x.dr.at[slot], partner).start()

    def moments(x, kind, r):
        slot = lax.rem(r, LOADS)
        layer, rows, cols = piece(x.which, r)
        pltpu.make_async_copy(x.w.at[layer, own, c, rows, cols], x.wl.at[slot], x.mo.at[slot, 0]).start()
        pltpu.make_async_copy(mine(x, x.m, r), x.ml.at[slot], x.mo.at[slot, 1]).start()
        pltpu.make_async_copy(mine(x, x.v, r), x.vl.at[slot], x.mo.at[slot, 2]).start()

    def along(x, r, slot, row, k, base, *terms):
        j = row * 4 + e[k]
        to = base + e_slot[k]
        send(x.s.at[slot, j], x.rb.at[r, to], x.ss.at[slot], x.rr.at[r, to], e_to[k]).start()

    def first(x, kind, r):
        slot = lax.rem(r, SLOTS)
        pltpu.make_async_copy(blocks(x, x.g, r, slice(None), c), x.s.at[slot], x.ld.at[slot]).wait()
        arrive(x.d.at[slot], x.dr.at[slot])
        if kind == "y":
            for col in (*e, z):
                j = (1 - y) * 4 + col
                add(x, x.s.at[slot, j], x.s.at[slot, j], x.d.at[slot, j])
                send(x.s.at[slot, j], x.rb.at[r, col], x.ss.at[slot], x.rr.at[r, col], across).start()
        else:

            @pl.when(corner)
            def _():
                for row in (1 - y, y):
                    for k in range(3):
                        j = row * 4 + e[k]
                        add(x, x.s.at[slot, j], x.s.at[slot, j], x.d.at[slot, j])
                        along(x, r, slot, row, k, row * 5)

    def hops(x, kind, r, ks):
        slot = lax.rem(r, SLOTS)
        if kind == "y":
            for k in ks:
                j = y * 4 + e[k]
                arrive(x.rb.at[r, e[k]], x.rr.at[r, e[k]])

                @pl.when(mid)
                def _():
                    arrive(x.rb.at[r, 4 + e[k]], x.rr.at[r, 4 + e[k]])
                    add(x, x.s.at[slot, j], x.s.at[slot, j], x.d.at[slot, j], x.rb.at[r, e[k]], x.rb.at[r, 4 + e[k]])

                @pl.when(corner)
                def _():
                    add(x, x.s.at[slot, j], x.s.at[slot, j], x.d.at[slot, j], x.rb.at[r, e[k]])

                along(x, r, slot, y, k, 4)
        else:

            @pl.when(mid)
            def _():
                for row in (1 - y, y):
                    for k in ks:
                        j = row * 4 + e[k]
                        at = row * 5 + e[k]
                        arrive(x.rb.at[r, at], x.rr.at[r, at])
                        add(x, x.s.at[slot, j], x.s.at[slot, j], x.d.at[slot, j], x.rb.at[r, at])
                        along(x, r, slot, row, k, row * 5)

    def near(x, kind, r):
        hops(x, kind, r, (0, 1))

    def far(x, kind, r):
        hops(x, kind, r, (2,))

    def cross(x, kind, r):
        slot = lax.rem(r, SLOTS)
        j = (1 - y) * 4 + z
        ends(x, r, (1 - y) * 5)(lambda *got: add(x, x.s.at[slot, j], x.s.at[slot, j], x.d.at[slot, j], *got))
        send(x.s.at[slot, j], x.rb.at[r, 10], x.ss.at[slot], x.rr.at[r, 10], across).start()

    def share(x, kind, r, src, j, to_y, to_z):
        dst = blocks(x, x.out, r, j, c)
        t = 0 if kind == "y" else 1
        if to_y:
            send(src, dst, x.ay.at[t], x.ar.at[r, j], across).start()
        if to_z:

            @pl.when(z < 3)
            def _():
                send(src, dst, x.az.at[t], x.ar.at[r, j], me + 2).start()

            @pl.when(z > 0)
            def _():
                send(src, dst, x.az.at[t], x.ar.at[r, j], me - 2).start()

        send(src, dst, x.ad, x.adr, partner).start()

    def step(x, kind, r):
        slot, at = lax.rem(r, SLOTS), lax.rem(r, LOADS)
        over = z if kind == "y" else 10
        arrive(x.rb.at[r, over], x.rr.at[r, over])
        base = 4 if kind == "y" else y * 5
        ends(x, r, base)(lambda *got: add(x, x.gb.at[r], x.s.at[slot, own], x.d.at[slot, own], x.rb.at[r, over], *got))
        layer, rows, cols = piece(x.which, r)
        pltpu.make_async_copy(x.w.at[layer, own, c, rows, cols], x.wl.at[at], x.mo.at[at, 0]).wait()
        pltpu.make_async_copy(mine(x, x.m, r), x.ml.at[at], x.mo.at[at, 1]).wait()
        pltpu.make_async_copy(mine(x, x.v, r), x.vl.at[at], x.mo.at[at, 2]).wait()

        def slab(k, carry):
            rows = pl.ds(pl.multiple_of(k * 16, 16), 16)
            m, v = new_moments(x.ml[at, rows, :], x.vl[at, rows, :], x.gb[r, rows, :].astype(jnp.float32))
            x.wb[r, rows, :] = new_weight(x.wl[at, rows, :].astype(jnp.float32), m, v)
            return carry

        lax.fori_loop(0, shape_of(x.which)[0] // 16, slab, 0)
        share(x, kind, r, x.wb.at[r], own, True, True)
        pltpu.make_async_copy(x.wb.at[r], blocks(x, x.out, r, own, c), x.lo).start()
        pltpu.make_async_copy(x.gb.at[r], mine(x, x.gout, r), x.lo).start()

        @pl.when(r < ROUNDS - SLOTS)
        def _():
            pl.semaphore_signal(x.free, inc=1, device_id=(rep, partner), device_id_type=MESH)

    def came(x, r, j):
        arrive(blocks(x, x.out, r, j, c), x.ar.at[r, j])
        return blocks(x, x.out, r, j, c)

    def pass0(x, kind, r):
        j = (1 - y) * 4 + z
        share(x, kind, r, came(x, r, j), j, False, True)

    def passes(x, kind, r, ks):
        t = 0 if kind == "y" else 1
        for row in (y,) if kind == "y" else (y, 1 - y):
            for k in ks:
                j = row * 4 + f[k]
                src = came(x, r, j)

                @pl.when(mid)
                def _():
                    send(src, src, x.az.at[t], x.ar.at[r, j], f_to[k]).start()

                share(x, kind, r, src, j, kind == "y", False)

    def pass1(x, kind, r):
        passes(x, kind, r, (0, 1))

    def pass2(x, kind, r):
        passes(x, kind, r, (2,))

    def pass3(x, kind, r):
        for col in (z, *f):
            j = (1 - y) * 4 + col
            share(x, kind, r, came(x, r, j), j, False, False)

    stages = {one.__name__: one for one in (fetch, moments, first, near, far, cross, step, pass0, pass1, pass2, pass3)}

    barrier = pltpu.get_barrier_semaphore()
    pl.semaphore_signal(barrier, inc=1, device_id=(rep, partner), device_id_type=MESH)
    pl.semaphore_signal(barrier, inc=1, device_id=(rep, across), device_id_type=MESH)

    @pl.when(z < 3)
    def _():
        pl.semaphore_signal(barrier, inc=1, device_id=(rep, me + 2), device_id_type=MESH)

    @pl.when(z > 0)
    def _():
        pl.semaphore_signal(barrier, inc=1, device_id=(rep, me - 2), device_id_type=MESH)

    @pl.when(mid)
    def _():
        pl.semaphore_wait(barrier, 4)

    @pl.when(corner)
    def _():
        pl.semaphore_wait(barrier, 3)

    def turn(i, carry):
        for sub in range(3):
            for name in ORDER:
                for kind in ("y", "z"):
                    lag = dict(LAGS[kind]).get(name)
                    if lag is None:
                        continue
                    x = weights[(sub - lag) % 3]
                    if kind not in x.types:
                        continue
                    r = i + (sub - lag) // 3
                    ok = (r >= 0) & (r < ROUNDS)
                    if len(set(x.types)) > 1:
                        last = lax.rem(r + 4, 4) == 3
                        ok = ok & (last if kind == "z" else jnp.logical_not(last))
                    pl.when(ok)(functools.partial(stages[name], x, kind, r))
        return carry

    longest = max(lag for kind in LAGS.values() for _, lag in kind)
    lax.fori_loop(0, ROUNDS + (longest + 2) // 3, turn, 0)

    for x in weights:
        for slot in range(SLOTS):
            left(x.s.at[slot, pl.ds(0, 7)], x.ss.at[slot])
        for t, kind in enumerate(("y", "z")):
            n = x.types.count(kind)
            if n:
                left(x.rb.at[pl.ds(0, n), pl.ds(0, 4 if kind == "y" else 1)], x.ay.at[t])

                @pl.when(mid)
                def _():
                    if kind == "y":
                        left(x.rb.at[pl.ds(0, n), pl.ds(0, 5)], x.az.at[t])
                    else:
                        left(x.rb.at[pl.ds(0, n), pl.ds(0, 10)], x.az.at[t])

                @pl.when(corner)
                def _():
                    left(x.rb.at[pl.ds(0, n), pl.ds(0, 1 if kind == "y" else 2)], x.az.at[t])

        left(x.rb.at[:, pl.ds(0, 8)], x.ds)
        left(x.rb.at[:, pl.ds(0, 8)], x.ad)
        arrive(x.rb.at[:, pl.ds(0, 8)], x.adr)
        arrive(x.rb.at[:, pl.ds(0, 2)], x.lo)


def solution(mesh):
    def step(*arrays):
        terms, weights, m, v = (arrays[i : i + 3] for i in (0, 3, 6, 9))

        def cut(one):
            rows, cols = one.shape[-2:]
            return one.reshape(2, 8, 2, rows // 16, cols)

        wide = [cut(one) for one in weights]
        outs = pl.pallas_call(
            kernel,
            out_shape=[jax.ShapeDtypeStruct(one.shape, jnp.bfloat16) for one in (*wide, *m)],
            in_specs=[ANY] * 12,
            out_specs=[ANY] * 6,
            scratch_shapes=[one for i in range(3) for one in scratch(i)],
            compiler_params=pltpu.CompilerParams(collective_id=0, has_side_effects=True, vmem_limit_bytes=67043328),
            name="sum_step_gather",
        )(*(cut(t[0]) for t in terms), *wide, *m, *v)
        whole = [one.reshape(w.shape) for one, w in zip(outs[:3], weights, strict=True)]
        new = [new_moments(*mvg) for mvg in zip(m, v, (g.astype(jnp.float32) for g in outs[3:]), strict=True)]
        return (*whole, *(one[0] for one in new), *(one[1] for one in new))

    all_of, cut = P(None, None, None), P(None, "dp", None)
    return jax.shard_map(
        step,
        mesh=mesh,
        in_specs=(P(("rep", "dp"), None, None, None),) * 3 + (all_of,) * 3 + (cut,) * 6,
        out_specs=(P("rep", None, None),) * 3 + (P("rep", "dp", None),) * 6,
        check_vma=False,
    )
```

```python
import functools

import jax
import jax.numpy as jnp
from jax import lax
from jax.experimental import pallas as pl
from jax.experimental.pallas import tpu as pltpu
from jax.sharding import PartitionSpec as P

MESH = pl.DeviceIdType.MESH
ANY = pl.BlockSpec(memory_space=pl.ANY)
ROUNDS = 16
SLOTS = 4
LOADS = 2
NAMES = ("gate", "up", "down")
TYPES = (("y",) * ROUNDS, ("z",) * ROUNDS, ("y", "y", "y", "z") * (ROUNDS // 4))
LAGS = {
    "y": {"fetch": 0, "first": 3, "outer": 4, "inner": 5, "last": 6, "moments": 5, "step": 7, "hop1": 8, "hop2": 9, "hop3": 10, "over": 11},
    "z": {"fetch": 0, "outer": 3, "inner": 4, "last": 5, "cross": 6, "moments": 5, "step": 7, "pass0": 8, "hop1": 9, "hop2": 10, "hop3": 11},
}
ORDER = ("fetch", "moments", "first", "outer", "inner", "last", "cross", "step", "pass0", "hop1", "hop2", "hop3", "over")
KEYS = ("s", "d", "rb", "wb", "gb", "wl", "ml", "vl", "ld", "dr", "ds", "ss", "rr", "ar", "ad", "ay", "az", "lo", "adr", "mo", "mw", "free")


def new_moments(m, v, g):
    return 0.9 * m + 0.1 * g, 0.95 * v + 0.05 * g * g


def new_weight(w, m, v):
    return (w - 0.02 * (m * lax.rsqrt(v + 1e-8) + 0.1 * w)).astype(jnp.bfloat16)


def piece(which, r):
    rows, cols = shape_of(which)
    across = (1024 if which == 2 else 3584) // cols
    layer, q = r // (ROUNDS // 2), lax.rem(r, ROUNDS // 2)
    return layer, pl.ds(pl.multiple_of(q // across * rows, rows), rows), pl.ds(pl.multiple_of(lax.rem(q, across) * cols, cols), cols)


def shape_of(which):
    return (112, 4096 // ROUNDS) if which == 2 else (16, 28672 // ROUNDS)


def scratch(which):
    rows, cols = shape_of(which)
    bf, f32, dma = jnp.bfloat16, jnp.float32, pltpu.SemaphoreType.DMA
    return (
        pltpu.VMEM((SLOTS, 8, rows, cols), bf),
        pltpu.VMEM((SLOTS, 8, rows, cols), bf),
        pltpu.VMEM((ROUNDS, 9 if which == 0 else 11, rows, cols), bf),
        pltpu.VMEM((ROUNDS, rows, cols), bf),
        pltpu.VMEM((rows, cols), bf),
        pltpu.VMEM((LOADS, rows, cols), bf),
        pltpu.VMEM((LOADS, rows, cols), f32),
        pltpu.VMEM((LOADS, rows, cols), f32),
        dma((SLOTS,)),
        dma((SLOTS,)),
        dma,
        dma((SLOTS,)),
        dma((ROUNDS, 11)),
        dma((ROUNDS, 8)),
        dma,
        dma((2,)),
        dma((2,)),
        dma,
        dma,
        dma((LOADS, 3)),
        dma((LOADS, 2)),
        pltpu.SemaphoreType.REGULAR,
    )


class Weight:
    pass


def kernel(*refs):
    rep, me = lax.axis_index("rep"), lax.axis_index("dp")
    y, z, c = me // 8, lax.rem(me // 2, 4), lax.rem(me, 2)
    own = me // 2
    partner, across = me + 1 - 2 * c, me + 8 - 16 * y
    mid = (z > 0) & (z < 3)
    corner = (z == 0) | (z == 3)
    low = 1 - z // 2
    odd = lax.rem(z, 2)
    onward = me + 4 * low - 2
    e = (3 * low, 1 + low, low * (1 - z) + (1 - low) * (5 - z))
    e_to = (onward, onward, me + 2 - 4 * odd)
    e_slot = (e[0], e[1] + z // 2 * (1 - odd) * (4 - e[1]), e[2] + odd * (4 - e[2]))
    f = (z + 1 - 2 * odd, 2 - z // 2, 3 * low)
    f_to = (onward, me + 2 - 4 * low, me + 2 - 4 * low)

    inputs, outputs, rest = refs[:12], refs[12:21], refs[21:]
    weights = []
    for i in range(3):
        x = Weight()
        x.which, x.types = i, TYPES[i]
        x.g, x.w, x.m, x.v = inputs[i], inputs[3 + i], inputs[6 + i], inputs[9 + i]
        x.out, x.mout, x.vout = outputs[i], outputs[3 + i], outputs[6 + i]
        for key, ref in zip(KEYS, rest[i * len(KEYS) : (i + 1) * len(KEYS)], strict=True):
            setattr(x, key, ref)
        weights.append(x)

    def send(src, dst, sent, got, to):
        return pltpu.make_async_remote_copy(src_ref=src, dst_ref=dst, send_sem=sent, recv_sem=got, device_id=(rep, to), device_id_type=MESH)

    def arrive(ref, sem):
        send(ref, ref, sem, sem, partner).wait_recv()

    def left(ref, sem):
        send(ref, ref, sem, sem, partner).wait_send()

    def blocks(x, ref, r, j, core):
        layer, rows, cols = piece(x.which, r)
        return ref.at[layer, j, core, rows, cols]

    def mine(x, ref, r):
        layer, rows, cols = piece(x.which, r)
        return ref.at[layer, rows, cols]

    def add(x, dst, *terms):
        total = terms[0][...].astype(jnp.float32)
        for term in terms[1:]:
            total += term[...].astype(jnp.float32)
        dst[...] = total.astype(jnp.bfloat16)

    def ends(x, r, base):
        def when(then):
            @pl.when(mid)
            def _():
                arrive(x.rb.at[r, base + z], x.rr.at[r, base + z])
                arrive(x.rb.at[r, base + 4], x.rr.at[r, base + 4])
                then(x.rb.at[r, base + z], x.rb.at[r, base + 4])

            @pl.when(corner)
            def _():
                at = base + 4 - z // 3
                arrive(x.rb.at[r, at], x.rr.at[r, at])
                then(x.rb.at[r, at])

        return when

    def fetch(x, kind, r):
        slot = lax.rem(r, SLOTS)

        @pl.when(r >= SLOTS)
        def _():
            left(x.s.at[slot, pl.ds(0, 7)], x.ss.at[slot])
            pl.semaphore_wait(x.free, 1)

        pltpu.make_async_copy(blocks(x, x.g, r, slice(None), c), x.s.at[slot], x.ld.at[slot]).start()
        send(blocks(x, x.g, r, slice(None), 1 - c), x.d.at[slot], x.ds, x.dr.at[slot], partner).start()

    def written(x, r, slot):
        return (
            pltpu.make_async_copy(x.ml.at[slot], mine(x, x.mout, r), x.mw.at[slot, 0]),
            pltpu.make_async_copy(x.vl.at[slot], mine(x, x.vout, r), x.mw.at[slot, 1]),
        )

    def moments(x, kind, r):
        slot = lax.rem(r, LOADS)
        layer, rows, cols = piece(x.which, r)

        @pl.when(r >= LOADS)
        def _():
            for one in written(x, r, slot):
                one.wait()

        pltpu.make_async_copy(x.w.at[layer, own, c, rows, cols], x.wl.at[slot], x.mo.at[slot, 0]).start()
        pltpu.make_async_copy(mine(x, x.m, r), x.ml.at[slot], x.mo.at[slot, 1]).start()
        pltpu.make_async_copy(mine(x, x.v, r), x.vl.at[slot], x.mo.at[slot, 2]).start()

    def along(x, r, slot, row, k, base, *terms):
        j = row * 4 + e[k]
        to = base + e_slot[k]
        send(x.s.at[slot, j], x.rb.at[r, to], x.ss.at[slot], x.rr.at[r, to], e_to[k]).start()

    def ready(x, r, slot):
        pltpu.make_async_copy(blocks(x, x.g, r, slice(None), c), x.s.at[slot], x.ld.at[slot]).wait()
        arrive(x.d.at[slot], x.dr.at[slot])

    def first(x, kind, r):
        slot = lax.rem(r, SLOTS)
        ready(x, r, slot)
        for col in (*e, z):
            j = (1 - y) * 4 + col
            add(x, x.s.at[slot, j], x.s.at[slot, j], x.d.at[slot, j])
            send(x.s.at[slot, j], x.rb.at[r, col], x.ss.at[slot], x.rr.at[r, col], across).start()

    def onto(x, kind, r, ks, inner):
        slot = lax.rem(r, SLOTS)
        for row in (y,) if kind == "y" else (1 - y, y):
            base = 4 if kind == "y" else row * 5
            for k in ks:
                j = row * 4 + e[k]
                terms = [x.s.at[slot, j], x.d.at[slot, j]]
                if kind == "y":
                    arrive(x.rb.at[r, e[k]], x.rr.at[r, e[k]])
                    terms.append(x.rb.at[r, e[k]])
                if inner:
                    arrive(x.rb.at[r, base + e[k]], x.rr.at[r, base + e[k]])
                    terms.append(x.rb.at[r, base + e[k]])
                add(x, x.s.at[slot, j], *terms)
                along(x, r, slot, row, k, base)

    def outer(x, kind, r):
        if kind == "z":
            ready(x, r, lax.rem(r, SLOTS))
        pl.when(corner)(lambda: onto(x, kind, r, (0, 1, 2), False))

    def inner(x, kind, r):
        pl.when(mid)(lambda: onto(x, kind, r, (0, 1), True))

    def last(x, kind, r):
        pl.when(mid)(lambda: onto(x, kind, r, (2,), True))

    def cross(x, kind, r):
        slot = lax.rem(r, SLOTS)
        j = (1 - y) * 4 + z
        ends(x, r, (1 - y) * 5)(lambda *got: add(x, x.s.at[slot, j], x.s.at[slot, j], x.d.at[slot, j], *got))
        send(x.s.at[slot, j], x.rb.at[r, 10], x.ss.at[slot], x.rr.at[r, 10], across).start()

    def share(x, kind, r, src, j, to_y, to_z):
        dst = blocks(x, x.out, r, j, c)
        t = 0 if kind == "y" else 1
        if to_y:
            send(src, dst, x.ay.at[t], x.ar.at[r, j], across).start()
        if to_z:

            @pl.when(z < 3)
            def _():
                send(src, dst, x.az.at[t], x.ar.at[r, j], me + 2).start()

            @pl.when(z > 0)
            def _():
                send(src, dst, x.az.at[t], x.ar.at[r, j], me - 2).start()

        send(src, dst, x.ad, x.adr, partner).start()

    def step(x, kind, r):
        slot, at = lax.rem(r, SLOTS), lax.rem(r, LOADS)
        over = z if kind == "y" else 10
        arrive(x.rb.at[r, over], x.rr.at[r, over])
        base = 4 if kind == "y" else y * 5
        ends(x, r, base)(lambda *got: add(x, x.gb, x.s.at[slot, own], x.d.at[slot, own], x.rb.at[r, over], *got))
        layer, rows, cols = piece(x.which, r)
        pltpu.make_async_copy(x.w.at[layer, own, c, rows, cols], x.wl.at[at], x.mo.at[at, 0]).wait()
        pltpu.make_async_copy(mine(x, x.m, r), x.ml.at[at], x.mo.at[at, 1]).wait()
        pltpu.make_async_copy(mine(x, x.v, r), x.vl.at[at], x.mo.at[at, 2]).wait()

        m, v = new_moments(x.ml[at], x.vl[at], x.gb[...].astype(jnp.float32))
        x.ml[at] = m
        x.vl[at] = v
        x.wb[r] = new_weight(x.wl[at].astype(jnp.float32), m, v)
        share(x, kind, r, x.wb.at[r], own, True, True)
        pltpu.make_async_copy(x.wb.at[r], blocks(x, x.out, r, own, c), x.lo).start()
        for one in written(x, r, at):
            one.start()

        @pl.when(r < ROUNDS - SLOTS)
        def _():
            pl.semaphore_signal(x.free, inc=1, device_id=(rep, partner), device_id_type=MESH)

    def came(x, r, j):
        arrive(blocks(x, x.out, r, j, c), x.ar.at[r, j])
        return blocks(x, x.out, r, j, c)

    def pass0(x, kind, r):
        j = (1 - y) * 4 + z
        share(x, kind, r, came(x, r, j), j, False, True)

    def passes(x, kind, r, ks, inner):
        t = 0 if kind == "y" else 1
        for row in (y,) if kind == "y" else (y, 1 - y):
            for k in ks:
                j = row * 4 + f[k]
                src = came(x, r, j)
                if inner:
                    send(src, src, x.az.at[t], x.ar.at[r, j], f_to[k]).start()
                share(x, kind, r, src, j, kind == "y", False)

    def hop1(x, kind, r):
        pl.when(mid)(lambda: passes(x, kind, r, (0, 1), True))
        pl.when(corner)(lambda: passes(x, kind, r, (0,), False))

    def hop2(x, kind, r):
        pl.when(mid)(lambda: passes(x, kind, r, (2,), True))
        pl.when(corner)(lambda: passes(x, kind, r, (1,), False))

    def hop3(x, kind, r):
        pl.when(corner)(lambda: passes(x, kind, r, (2,), False))

    def over(x, kind, r):
        for col in (z, *f):
            j = (1 - y) * 4 + col
            share(x, kind, r, came(x, r, j), j, False, False)

    stages = {one.__name__: one for one in (fetch, moments, first, outer, inner, last, cross, step, pass0, hop1, hop2, hop3, over)}

    barrier = pltpu.get_barrier_semaphore()
    pl.semaphore_signal(barrier, inc=1, device_id=(rep, partner), device_id_type=MESH)
    pl.semaphore_signal(barrier, inc=1, device_id=(rep, across), device_id_type=MESH)

    @pl.when(z < 3)
    def _():
        pl.semaphore_signal(barrier, inc=1, device_id=(rep, me + 2), device_id_type=MESH)

    @pl.when(z > 0)
    def _():
        pl.semaphore_signal(barrier, inc=1, device_id=(rep, me - 2), device_id_type=MESH)

    @pl.when(mid)
    def _():
        pl.semaphore_wait(barrier, 4)

    @pl.when(corner)
    def _():
        pl.semaphore_wait(barrier, 3)

    def turn(i, carry):
        for sub in range(3):
            for name in ORDER:
                for kind in ("y", "z"):
                    lag = LAGS[kind].get(name)
                    if lag is None:
                        continue
                    x = weights[(sub - lag) % 3]
                    if kind not in x.types:
                        continue
                    r = i + (sub - lag) // 3
                    ok = (r >= 0) & (r < ROUNDS)
                    if len(set(x.types)) > 1:
                        last = lax.rem(r + 4, 4) == 3
                        ok = ok & (last if kind == "z" else jnp.logical_not(last))
                    pl.when(ok)(functools.partial(stages[name], x, kind, r))
        return carry

    longest = max(max(kind.values()) for kind in LAGS.values())
    lax.fori_loop(0, ROUNDS + (longest + 2) // 3, turn, 0)

    for x in weights:
        for slot in range(SLOTS):
            left(x.s.at[slot, pl.ds(0, 7)], x.ss.at[slot])
        for t, kind in enumerate(("y", "z")):
            n = x.types.count(kind)
            if n:
                left(x.rb.at[pl.ds(0, n), pl.ds(0, 4 if kind == "y" else 1)], x.ay.at[t])

                @pl.when(mid)
                def _():
                    if kind == "y":
                        left(x.rb.at[pl.ds(0, n), pl.ds(0, 5)], x.az.at[t])
                    else:
                        left(x.rb.at[pl.ds(0, n), pl.ds(0, 10)], x.az.at[t])

                @pl.when(corner)
                def _():
                    left(x.rb.at[pl.ds(0, n), pl.ds(0, 1 if kind == "y" else 2)], x.az.at[t])

        left(x.rb.at[:, pl.ds(0, 8)], x.ds)
        left(x.rb.at[:, pl.ds(0, 8)], x.ad)
        arrive(x.rb.at[:, pl.ds(0, 8)], x.adr)
        arrive(x.rb.at[:, pl.ds(0, 1)], x.lo)
        for r in range(ROUNDS - LOADS, ROUNDS):
            for one in written(x, jnp.int32(r), r % LOADS):
                one.wait()


def solution(mesh):
    def step(*arrays):
        terms, weights, m, v = (arrays[i : i + 3] for i in (0, 3, 6, 9))

        def cut(one):
            rows, cols = one.shape[-2:]
            return one.reshape(2, 8, 2, rows // 16, cols)

        wide = [cut(one) for one in weights]
        outs = pl.pallas_call(
            kernel,
            out_shape=[jax.ShapeDtypeStruct(one.shape, one.dtype) for one in (*wide, *m, *v)],
            in_specs=[ANY] * 12,
            out_specs=[ANY] * 9,
            scratch_shapes=[one for i in range(3) for one in scratch(i)],
            compiler_params=pltpu.CompilerParams(collective_id=0, has_side_effects=True, vmem_limit_bytes=67043328),
            name="sum_step_gather",
        )(*(cut(t[0]) for t in terms), *wide, *m, *v)
        whole = [one.reshape(w.shape) for one, w in zip(outs[:3], weights, strict=True)]
        return (*whole, *outs[3:])

    all_of, cut = P(None, None, None), P(None, "dp", None)
    return jax.shard_map(
        step,
        mesh=mesh,
        in_specs=(P(("rep", "dp"), None, None, None),) * 3 + (all_of,) * 3 + (cut,) * 6,
        out_specs=(P("rep", None, None),) * 3 + (P("rep", "dp", None),) * 6,
        check_vma=False,
    )
```

```python
import functools

import jax
import jax.numpy as jnp
from jax import lax
from jax.experimental import pallas as pl
from jax.experimental.pallas import tpu as pltpu
from jax.sharding import PartitionSpec as P

MESH = pl.DeviceIdType.MESH
ANY = pl.BlockSpec(memory_space=pl.ANY)
ROUNDS = 32
SLOTS = 5
INBOX = 5
HELD = (False, False, False)
LOADS = 2
NAMES = ("gate", "up", "down")
TYPES = (("y",) * ROUNDS, ("z",) * ROUNDS, ("y", "y", "y", "z") * (ROUNDS // 4))
LAGS = {
    "y": {"fetch": 0, "first": 2, "outer": 4, "inner": 6, "last": 8, "moments": 7, "step": 10, "hop1": 12, "hop2": 14, "hop3": 16, "over": 18},
    "z": {"fetch": 0, "outer": 2, "inner": 4, "last": 6, "cross": 8, "moments": 7, "step": 10, "pass0": 12, "hop1": 14, "hop2": 16, "hop3": 18},
}
ORDER = ("fetch", "moments", "first", "outer", "inner", "last", "cross", "step", "pass0", "hop1", "hop2", "hop3", "over")
KEYS = ("s", "d", "rb", "wb", "gb", "wl", "ml", "vl", "ld", "dr", "ds", "ss", "rr", "ar", "ad", "ay", "az", "adr", "mo", "mw", "lo", "free", "y_free", "on_free", "back_free")


def new_moments(m, v, g):
    return 0.9 * m + 0.1 * g, 0.95 * v + 0.05 * g * g


def new_weight(w, m, v):
    return (w - 0.02 * (m * lax.rsqrt(v + 1e-8) + 0.1 * w)).astype(jnp.bfloat16)


def piece(which, r):
    rows, cols = shape_of(which)
    across = (1024 if which == 2 else 3584) // cols
    layer, q = r // (ROUNDS // 2), lax.rem(r, ROUNDS // 2)
    return layer, pl.ds(pl.multiple_of(q // across * rows, rows), rows), pl.ds(pl.multiple_of(lax.rem(q, across) * cols, cols), cols)


def shape_of(which):
    return (112, 4096 // ROUNDS) if which == 2 else (16, 28672 // ROUNDS)


def block_of(which):
    return (224, 1024) if which == 2 else (64, 3584)


def scratch(which):
    rows, cols = shape_of(which)
    bf, f32, dma = jnp.bfloat16, jnp.float32, pltpu.SemaphoreType.DMA
    return (
        pltpu.VMEM((SLOTS, 8, rows, cols), bf),
        pltpu.VMEM((SLOTS, 8, rows, cols), bf),
        pltpu.VMEM((INBOX, 9 if which == 0 else 11, rows, cols), bf),
        pltpu.VMEM((1 if HELD[which] else ROUNDS, rows, cols), bf),
        pltpu.VMEM((rows, cols), bf),
        pltpu.VMEM((LOADS, rows, cols), bf),
        pltpu.VMEM((LOADS, rows, cols), f32),
        pltpu.VMEM((LOADS, rows, cols), f32),
        dma((SLOTS,)),
        dma((SLOTS,)),
        dma,
        dma((SLOTS,)),
        dma((INBOX, 11)),
        dma((ROUNDS, 8)),
        dma,
        dma((2,)),
        dma((2,)),
        dma,
        dma((LOADS, 3)),
        dma((LOADS, 2)),
        dma,
        *([pltpu.SemaphoreType.REGULAR] * 4),
    )


class Weight:
    pass


def kernel(*refs):
    rep, me = lax.axis_index("rep"), lax.axis_index("dp")
    y, z, c = me // 8, lax.rem(me // 2, 4), lax.rem(me, 2)
    own = me // 2
    partner, across = me + 1 - 2 * c, me + 8 - 16 * y
    mid = (z > 0) & (z < 3)
    corner = (z == 0) | (z == 3)
    low = 1 - z // 2
    odd = lax.rem(z, 2)
    onward = me + 4 * low - 2
    e = (3 * low, 1 + low, low * (1 - z) + (1 - low) * (5 - z))
    e_to = (onward, onward, me + 2 - 4 * odd)
    e_slot = (e[0], e[1] + z // 2 * (1 - odd) * (4 - e[1]), e[2] + odd * (4 - e[2]))
    f = (z + 1 - 2 * odd, 2 - z // 2, 3 * low)
    f_to = (onward, me + 2 - 4 * low, me + 2 - 4 * low)

    inputs, outputs, rest = refs[:12], refs[12:21], refs[21:]
    weights = []
    for i in range(3):
        x = Weight()
        x.which, x.types = i, TYPES[i]
        x.g, x.w, x.m, x.v = inputs[i], inputs[3 + i], inputs[6 + i], inputs[9 + i]
        x.out, x.mout, x.vout = outputs[i], outputs[3 + i], outputs[6 + i]
        for key, ref in zip(KEYS, rest[i * len(KEYS) : (i + 1) * len(KEYS)], strict=True):
            setattr(x, key, ref)
        weights.append(x)

    def send(src, dst, sent, got, to):
        return pltpu.make_async_remote_copy(src_ref=src, dst_ref=dst, send_sem=sent, recv_sem=got, device_id=(rep, to), device_id_type=MESH)

    def arrive(ref, sem):
        send(ref, ref, sem, sem, partner).wait_recv()

    def left(ref, sem):
        send(ref, ref, sem, sem, partner).wait_send()

    def blocks(x, ref, r, j, core):
        layer, rows, cols = piece(x.which, r)
        return ref.at[layer, j, core, rows, cols]

    def mine(x, ref, r):
        layer, rows, cols = piece(x.which, r)
        return ref.at[layer, rows, cols]

    def add(x, dst, *terms):
        total = terms[0][...].astype(jnp.float32)
        for term in terms[1:]:
            total += term[...].astype(jnp.float32)
        dst[...] = total.astype(jnp.bfloat16)

    def ends(x, r, base):
        def when(then):
            @pl.when(mid)
            def _():
                arrive(x.rb.at[lax.rem(r, INBOX), base + z], x.rr.at[lax.rem(r, INBOX), base + z])
                arrive(x.rb.at[lax.rem(r, INBOX), base + 4], x.rr.at[lax.rem(r, INBOX), base + 4])
                then(x.rb.at[lax.rem(r, INBOX), base + z], x.rb.at[lax.rem(r, INBOX), base + 4])

            @pl.when(corner)
            def _():
                at = base + 4 - z // 3
                arrive(x.rb.at[lax.rem(r, INBOX), at], x.rr.at[lax.rem(r, INBOX), at])
                then(x.rb.at[lax.rem(r, INBOX), at])

        return when

    def fetch(x, kind, r):
        slot = lax.rem(r, SLOTS)

        @pl.when(r >= SLOTS)
        def _():
            left(x.s.at[slot, pl.ds(0, 7)], x.ss.at[slot])
            pl.semaphore_wait(x.free, 1)

        pltpu.make_async_copy(blocks(x, x.g, r, slice(None), c), x.s.at[slot], x.ld.at[slot]).start()
        send(blocks(x, x.g, r, slice(None), 1 - c), x.d.at[slot], x.ds, x.dr.at[slot], partner).start()

    def written(x, r, slot):
        return (
            pltpu.make_async_copy(x.ml.at[slot], mine(x, x.mout, r), x.mw.at[slot, 0]),
            pltpu.make_async_copy(x.vl.at[slot], mine(x, x.vout, r), x.mw.at[slot, 1]),
        )

    def moments(x, kind, r):
        slot = lax.rem(r, LOADS)
        layer, rows, cols = piece(x.which, r)

        @pl.when(r >= LOADS)
        def _():
            for one in written(x, r, slot):
                one.wait()

        pltpu.make_async_copy(x.w.at[layer, own, c, rows, cols], x.wl.at[slot], x.mo.at[slot, 0]).start()
        pltpu.make_async_copy(mine(x, x.m, r), x.ml.at[slot], x.mo.at[slot, 1]).start()
        pltpu.make_async_copy(mine(x, x.v, r), x.vl.at[slot], x.mo.at[slot, 2]).start()

    def along(x, r, slot, row, k, base, *terms):
        j = row * 4 + e[k]
        to = base + e_slot[k]
        send(x.s.at[slot, j], x.rb.at[lax.rem(r, INBOX), to], x.ss.at[slot], x.rr.at[lax.rem(r, INBOX), to], e_to[k]).start()

    def ready(x, r, slot):
        pltpu.make_async_copy(blocks(x, x.g, r, slice(None), c), x.s.at[slot], x.ld.at[slot]).wait()
        arrive(x.d.at[slot], x.dr.at[slot])

    def granted(r, free):
        pl.when(r >= INBOX)(lambda: pl.semaphore_wait(free, 1))

    def grant(free, to):
        pl.semaphore_signal(free, inc=1, device_id=(rep, to), device_id_type=MESH)

    def first(x, kind, r):
        slot = lax.rem(r, SLOTS)
        ready(x, r, slot)
        granted(r, x.y_free)
        for col in (*e, z):
            j = (1 - y) * 4 + col
            add(x, x.s.at[slot, j], x.s.at[slot, j], x.d.at[slot, j])
            send(x.s.at[slot, j], x.rb.at[lax.rem(r, INBOX), col], x.ss.at[slot], x.rr.at[lax.rem(r, INBOX), col], across).start()

    def onto(x, kind, r, ks, inner):
        slot = lax.rem(r, SLOTS)
        for row in (y,) if kind == "y" else (1 - y, y):
            base = 4 if kind == "y" else row * 5
            for k in ks:
                j = row * 4 + e[k]
                terms = [x.s.at[slot, j], x.d.at[slot, j]]
                if kind == "y":
                    arrive(x.rb.at[lax.rem(r, INBOX), e[k]], x.rr.at[lax.rem(r, INBOX), e[k]])
                    terms.append(x.rb.at[lax.rem(r, INBOX), e[k]])
                if inner:
                    arrive(x.rb.at[lax.rem(r, INBOX), base + e[k]], x.rr.at[lax.rem(r, INBOX), base + e[k]])
                    terms.append(x.rb.at[lax.rem(r, INBOX), base + e[k]])
                add(x, x.s.at[slot, j], *terms)
                along(x, r, slot, row, k, base)

    def outer(x, kind, r):
        if kind == "z":
            ready(x, r, lax.rem(r, SLOTS))

        @pl.when(corner)
        def _():
            granted(r, x.on_free)
            onto(x, kind, r, (0, 1, 2), False)

    def inner(x, kind, r):
        @pl.when(mid)
        def _():
            granted(r, x.on_free)
            onto(x, kind, r, (0, 1), True)

    def last(x, kind, r):
        @pl.when(mid)
        def _():
            granted(r, x.back_free)
            onto(x, kind, r, (2,), True)

    def cross(x, kind, r):
        slot = lax.rem(r, SLOTS)
        j = (1 - y) * 4 + z
        ends(x, r, (1 - y) * 5)(lambda *got: add(x, x.s.at[slot, j], x.s.at[slot, j], x.d.at[slot, j], *got))
        granted(r, x.y_free)
        send(x.s.at[slot, j], x.rb.at[lax.rem(r, INBOX), 10], x.ss.at[slot], x.rr.at[lax.rem(r, INBOX), 10], across).start()

    def share(x, kind, r, src, j, to_y, to_z):
        dst = blocks(x, x.out, r, j, c)
        t = 0 if kind == "y" else 1
        if to_y:
            send(src, dst, x.ay.at[t], x.ar.at[r, j], across).start()
        if to_z:

            @pl.when(z < 3)
            def _():
                send(src, dst, x.az.at[t], x.ar.at[r, j], me + 2).start()

            @pl.when(z > 0)
            def _():
                send(src, dst, x.az.at[t], x.ar.at[r, j], me - 2).start()

        send(src, dst, x.ad, x.adr, partner).start()

    def step(x, kind, r):
        slot, at = lax.rem(r, SLOTS), lax.rem(r, LOADS)
        over = z if kind == "y" else 10
        arrive(x.rb.at[lax.rem(r, INBOX), over], x.rr.at[lax.rem(r, INBOX), over])
        base = 4 if kind == "y" else y * 5
        ends(x, r, base)(lambda *got: add(x, x.gb, x.s.at[slot, own], x.d.at[slot, own], x.rb.at[lax.rem(r, INBOX), over], *got))
        layer, rows, cols = piece(x.which, r)
        pltpu.make_async_copy(x.w.at[layer, own, c, rows, cols], x.wl.at[at], x.mo.at[at, 0]).wait()
        pltpu.make_async_copy(mine(x, x.m, r), x.ml.at[at], x.mo.at[at, 1]).wait()
        pltpu.make_async_copy(mine(x, x.v, r), x.vl.at[at], x.mo.at[at, 2]).wait()

        m, v = new_moments(x.ml[at], x.vl[at], x.gb[...].astype(jnp.float32))
        x.ml[at] = m
        x.vl[at] = v
        layer, rows, cols = piece(x.which, r)
        new, place = new_weight(x.wl[at].astype(jnp.float32), m, v), blocks(x, x.out, r, own, c)
        if HELD[x.which]:
            x.out[layer, own, c, rows, cols] = new
            share(x, kind, r, place, own, True, True)
        else:
            x.wb[r] = new
            share(x, kind, r, x.wb.at[r], own, True, True)
            pltpu.make_async_copy(x.wb.at[r], place, x.lo).start()
        for one in written(x, r, at):
            one.start()

        pl.when(r < ROUNDS - SLOTS)(lambda: grant(x.free, partner))

        @pl.when(r < ROUNDS - INBOX)
        def _():
            grant(x.y_free, across)

            @pl.when(mid)
            def _():
                grant(x.on_free, onward)
                grant(x.on_free, 2 * me - onward)

            @pl.when(corner)
            def _():
                grant(x.back_free, onward)

    def came(x, r, j):
        arrive(blocks(x, x.out, r, j, c), x.ar.at[r, j])
        return blocks(x, x.out, r, j, c)

    def pass0(x, kind, r):
        j = (1 - y) * 4 + z
        share(x, kind, r, came(x, r, j), j, False, True)

    def passes(x, kind, r, ks, inner):
        t = 0 if kind == "y" else 1
        for row in (y,) if kind == "y" else (y, 1 - y):
            for k in ks:
                j = row * 4 + f[k]
                src = came(x, r, j)
                if inner:
                    send(src, src, x.az.at[t], x.ar.at[r, j], f_to[k]).start()
                share(x, kind, r, src, j, kind == "y", False)

    def hop1(x, kind, r):
        pl.when(mid)(lambda: passes(x, kind, r, (0, 1), True))
        pl.when(corner)(lambda: passes(x, kind, r, (0,), False))

    def hop2(x, kind, r):
        pl.when(mid)(lambda: passes(x, kind, r, (2,), True))
        pl.when(corner)(lambda: passes(x, kind, r, (1,), False))

    def hop3(x, kind, r):
        pl.when(corner)(lambda: passes(x, kind, r, (2,), False))

    def over(x, kind, r):
        for col in (z, *f):
            j = (1 - y) * 4 + col
            share(x, kind, r, came(x, r, j), j, False, False)

    stages = {one.__name__: one for one in (fetch, moments, first, outer, inner, last, cross, step, pass0, hop1, hop2, hop3, over)}

    barrier = pltpu.get_barrier_semaphore()
    pl.semaphore_signal(barrier, inc=1, device_id=(rep, partner), device_id_type=MESH)
    pl.semaphore_signal(barrier, inc=1, device_id=(rep, across), device_id_type=MESH)

    @pl.when(z < 3)
    def _():
        pl.semaphore_signal(barrier, inc=1, device_id=(rep, me + 2), device_id_type=MESH)

    @pl.when(z > 0)
    def _():
        pl.semaphore_signal(barrier, inc=1, device_id=(rep, me - 2), device_id_type=MESH)

    @pl.when(mid)
    def _():
        pl.semaphore_wait(barrier, 4)

    @pl.when(corner)
    def _():
        pl.semaphore_wait(barrier, 3)

    def turn(i, carry):
        for sub in range(3):
            for name in ORDER:
                for kind in ("y", "z"):
                    lag = LAGS[kind].get(name)
                    if lag is None:
                        continue
                    x = weights[(sub - lag) % 3]
                    if kind not in x.types:
                        continue
                    r = i + (sub - lag) // 3
                    ok = (r >= 0) & (r < ROUNDS)
                    if len(set(x.types)) > 1:
                        last = lax.rem(r + 4, 4) == 3
                        ok = ok & (last if kind == "z" else jnp.logical_not(last))
                    pl.when(ok)(functools.partial(stages[name], x, kind, r))
        return carry

    longest = max(max(kind.values()) for kind in LAGS.values())
    lax.fori_loop(0, ROUNDS + (longest + 2) // 3, turn, 0)

    for x in weights:
        for slot in range(SLOTS):
            left(x.s.at[slot, pl.ds(0, 7)], x.ss.at[slot])
        for t, kind in enumerate(("y", "z")):
            share_of = block_of(x.which)[1] * x.types.count(kind) // ROUNDS
            if share_of:

                def all_of(k):
                    return x.out.at[:, pl.ds(0, k), 0, :, pl.ds(0, share_of)]

                left(all_of(4 if kind == "y" else 1), x.ay.at[t])

                @pl.when(mid)
                def _():
                    left(all_of(5) if kind == "y" else x.out.at[:, pl.ds(0, 5), :, :, pl.ds(0, share_of)], x.az.at[t])

                @pl.when(corner)
                def _():
                    left(all_of(1 if kind == "y" else 2), x.az.at[t])

        left(x.out.at[:, :, 0], x.ds)
        left(x.out.at[:, :, 0], x.ad)
        arrive(x.out.at[:, :, 0], x.adr)
        if not HELD[x.which]:
            arrive(x.wb, x.lo)
        for r in range(ROUNDS - LOADS, ROUNDS):
            for one in written(x, jnp.int32(r), r % LOADS):
                one.wait()


def solution(mesh):
    def step(*arrays):
        terms, weights, m, v = (arrays[i : i + 3] for i in (0, 3, 6, 9))

        def cut(one):
            rows, cols = one.shape[-2:]
            return one.reshape(2, 8, 2, rows // 16, cols)

        wide = [cut(one) for one in weights]
        outs = pl.pallas_call(
            kernel,
            out_shape=[*((pltpu.VMEM if held else jax.ShapeDtypeStruct)(one.shape, one.dtype) for held, one in zip(HELD, wide, strict=True)), *(pltpu.HBM(one.shape, one.dtype) for one in (*m, *v))],
            in_specs=[ANY] * 12,
            out_specs=[pl.BlockSpec(memory_space=pltpu.VMEM) if held else ANY for held in HELD] + [ANY] * 6,
            scratch_shapes=[one for i in range(3) for one in scratch(i)],
            compiler_params=pltpu.CompilerParams(collective_id=0, has_side_effects=True, vmem_limit_bytes=16 * 2**20),
            name="sum_step_gather",
        )(*(pltpu.with_memory_space_constraint(one, pltpu.HBM) for one in (*(cut(t[0]) for t in terms), *wide, *m, *v)))
        whole = [one.reshape(w.shape) for one, w in zip(outs[:3], weights, strict=True)]
        return (*whole, *outs[3:])

    all_of, cut = P(None, None, None), P(None, "dp", None)
    return jax.shard_map(
        step,
        mesh=mesh,
        in_specs=(P(("rep", "dp"), None, None, None),) * 3 + (all_of,) * 3 + (cut,) * 6,
        out_specs=(P("rep", None, None),) * 3 + (P("rep", "dp", None),) * 6,
        check_vma=False,
    )
```

```python
import functools

import jax
import jax.numpy as jnp
from jax import lax
from jax.experimental import pallas as pl
from jax.experimental.pallas import tpu as pltpu
from jax.sharding import PartitionSpec as P

MESH = pl.DeviceIdType.MESH
ANY = pl.BlockSpec(memory_space=pl.ANY)
ROUNDS = 32
SLOTS = 5
INBOX = 5
HELD = (False, False, False)
LOADS = 2
NAMES = ("gate", "up", "down")
ALONE = 6


def kinds(which, r, gather):
    among = r >= ALONE if not gather else r < ROUNDS - ALONE
    if which == 0:
        return ("y",), None
    if which == 1:
        return ("y", "z"), among | (lax.rem(r + ROUNDS, 2) == 1)
    return ("y", "z"), among & (lax.rem(r + ROUNDS, 4) == 3)


LAGS = {
    "y": {"fetch": 0, "first": 2, "outer": 4, "inner": 6, "last": 8, "moments": 7, "step": 10, "hop1": 12, "hop2": 14, "hop3": 16, "over": 18},
    "z": {"fetch": 0, "outer": 2, "inner": 4, "last": 6, "cross": 8, "moments": 7, "step": 10, "pass0": 12, "hop1": 14, "hop2": 16, "hop3": 18},
}
ORDER = ("fetch", "moments", "first", "outer", "inner", "last", "cross", "step", "pass0", "hop1", "hop2", "hop3", "over")
KEYS = ("s", "d", "rb", "wb", "gb", "wl", "ml", "vl", "ld", "dr", "ds", "ss", "rr", "ar", "ad", "ay", "az", "adr", "mo", "mw", "lo", "free", "y_free", "on_free", "back_free")


def new_moments(m, v, g):
    return 0.9 * m + 0.1 * g, 0.95 * v + 0.05 * g * g


def new_weight(w, m, v):
    return (w - 0.02 * (m * lax.rsqrt(v + 1e-8) + 0.1 * w)).astype(jnp.bfloat16)


def piece(which, r):
    rows, cols = shape_of(which)
    across = (1024 if which == 2 else 3584) // cols
    layer, q = r // (ROUNDS // 2), lax.rem(r, ROUNDS // 2)
    return layer, pl.ds(pl.multiple_of(q // across * rows, rows), rows), pl.ds(pl.multiple_of(lax.rem(q, across) * cols, cols), cols)


def shape_of(which):
    return (112, 4096 // ROUNDS) if which == 2 else (16, 28672 // ROUNDS)


def scratch(which):
    rows, cols = shape_of(which)
    bf, f32, dma = jnp.bfloat16, jnp.float32, pltpu.SemaphoreType.DMA
    return (
        pltpu.VMEM((SLOTS, 8, rows, cols), bf),
        pltpu.VMEM((SLOTS, 8, rows, cols), bf),
        pltpu.VMEM((INBOX, 9 if which == 0 else 11, rows, cols), bf),
        pltpu.VMEM((1 if HELD[which] else ROUNDS, rows, cols), bf),
        pltpu.VMEM((rows, cols), bf),
        pltpu.VMEM((LOADS, rows, cols), bf),
        pltpu.VMEM((LOADS, rows, cols), f32),
        pltpu.VMEM((LOADS, rows, cols), f32),
        dma((SLOTS,)),
        dma((SLOTS,)),
        dma,
        dma((SLOTS,)),
        dma((INBOX, 11)),
        dma((ROUNDS, 8)),
        dma,
        dma((ROUNDS,)),
        dma((ROUNDS,)),
        dma,
        dma((LOADS, 3)),
        dma((LOADS, 2)),
        dma,
        *([pltpu.SemaphoreType.REGULAR] * 4),
    )


class Weight:
    pass


GATHER = ("pass0", "hop1", "hop2", "hop3", "over")


def kernel(*refs):
    rep, me = lax.axis_index("rep"), lax.axis_index("dp")
    y, z, c = me // 8, lax.rem(me // 2, 4), lax.rem(me, 2)
    own = me // 2
    partner, across = me + 1 - 2 * c, me + 8 - 16 * y
    mid = (z > 0) & (z < 3)
    corner = (z == 0) | (z == 3)
    low = 1 - z // 2
    odd = lax.rem(z, 2)
    onward = me + 4 * low - 2
    e = (3 * low, 1 + low, low * (1 - z) + (1 - low) * (5 - z))
    e_to = (onward, onward, me + 2 - 4 * odd)
    e_slot = (e[0], e[1] + z // 2 * (1 - odd) * (4 - e[1]), e[2] + odd * (4 - e[2]))
    f = (z + 1 - 2 * odd, 2 - z // 2, 3 * low)
    f_to = (onward, me + 2 - 4 * low, me + 2 - 4 * low)

    inputs, outputs, rest = refs[:12], refs[12:21], refs[21:]
    weights = []
    for i in range(3):
        x = Weight()
        x.which = i
        x.g, x.w, x.m, x.v = inputs[i], inputs[3 + i], inputs[6 + i], inputs[9 + i]
        x.out, x.mout, x.vout = outputs[i], outputs[3 + i], outputs[6 + i]
        for key, ref in zip(KEYS, rest[i * len(KEYS) : (i + 1) * len(KEYS)], strict=True):
            setattr(x, key, ref)
        weights.append(x)

    def send(src, dst, sent, got, to):
        return pltpu.make_async_remote_copy(src_ref=src, dst_ref=dst, send_sem=sent, recv_sem=got, device_id=(rep, to), device_id_type=MESH)

    def arrive(ref, sem):
        send(ref, ref, sem, sem, partner).wait_recv()

    def left(ref, sem):
        send(ref, ref, sem, sem, partner).wait_send()

    def blocks(x, ref, r, j, core):
        layer, rows, cols = piece(x.which, r)
        return ref.at[layer, j, core, rows, cols]

    def mine(x, ref, r):
        layer, rows, cols = piece(x.which, r)
        return ref.at[layer, rows, cols]

    def add(x, dst, *terms):
        total = terms[0][...].astype(jnp.float32)
        for term in terms[1:]:
            total += term[...].astype(jnp.float32)
        dst[...] = total.astype(jnp.bfloat16)

    def ends(x, r, base):
        def when(then):
            @pl.when(mid)
            def _():
                arrive(x.rb.at[lax.rem(r, INBOX), base + z], x.rr.at[lax.rem(r, INBOX), base + z])
                arrive(x.rb.at[lax.rem(r, INBOX), base + 4], x.rr.at[lax.rem(r, INBOX), base + 4])
                then(x.rb.at[lax.rem(r, INBOX), base + z], x.rb.at[lax.rem(r, INBOX), base + 4])

            @pl.when(corner)
            def _():
                at = base + 4 - z // 3
                arrive(x.rb.at[lax.rem(r, INBOX), at], x.rr.at[lax.rem(r, INBOX), at])
                then(x.rb.at[lax.rem(r, INBOX), at])

        return when

    def fetch(x, kind, r):
        slot = lax.rem(r, SLOTS)

        @pl.when(r >= SLOTS)
        def _():
            left(x.s.at[slot, pl.ds(0, 7)], x.ss.at[slot])
            pl.semaphore_wait(x.free, 1)

        pltpu.make_async_copy(blocks(x, x.g, r, slice(None), c), x.s.at[slot], x.ld.at[slot]).start()
        send(blocks(x, x.g, r, slice(None), 1 - c), x.d.at[slot], x.ds, x.dr.at[slot], partner).start()

    def written(x, r, slot):
        return (
            pltpu.make_async_copy(x.ml.at[slot], mine(x, x.mout, r), x.mw.at[slot, 0]),
            pltpu.make_async_copy(x.vl.at[slot], mine(x, x.vout, r), x.mw.at[slot, 1]),
        )

    def moments(x, kind, r):
        slot = lax.rem(r, LOADS)
        layer, rows, cols = piece(x.which, r)

        @pl.when(r >= LOADS)
        def _():
            for one in written(x, r, slot):
                one.wait()

        pltpu.make_async_copy(x.w.at[layer, own, c, rows, cols], x.wl.at[slot], x.mo.at[slot, 0]).start()
        pltpu.make_async_copy(mine(x, x.m, r), x.ml.at[slot], x.mo.at[slot, 1]).start()
        pltpu.make_async_copy(mine(x, x.v, r), x.vl.at[slot], x.mo.at[slot, 2]).start()

    def along(x, r, slot, row, k, base, *terms):
        j = row * 4 + e[k]
        to = base + e_slot[k]
        send(x.s.at[slot, j], x.rb.at[lax.rem(r, INBOX), to], x.ss.at[slot], x.rr.at[lax.rem(r, INBOX), to], e_to[k]).start()

    def ready(x, r, slot):
        pltpu.make_async_copy(blocks(x, x.g, r, slice(None), c), x.s.at[slot], x.ld.at[slot]).wait()
        arrive(x.d.at[slot], x.dr.at[slot])

    def granted(r, free):
        pl.when(r >= INBOX)(lambda: pl.semaphore_wait(free, 1))

    def grant(free, to):
        pl.semaphore_signal(free, inc=1, device_id=(rep, to), device_id_type=MESH)

    def first(x, kind, r):
        slot = lax.rem(r, SLOTS)
        ready(x, r, slot)
        granted(r, x.y_free)
        for col in (*e, z):
            j = (1 - y) * 4 + col
            add(x, x.s.at[slot, j], x.s.at[slot, j], x.d.at[slot, j])
            send(x.s.at[slot, j], x.rb.at[lax.rem(r, INBOX), col], x.ss.at[slot], x.rr.at[lax.rem(r, INBOX), col], across).start()

    def onto(x, kind, r, ks, inner):
        slot = lax.rem(r, SLOTS)
        for row in (y,) if kind == "y" else (1 - y, y):
            base = 4 if kind == "y" else row * 5
            for k in ks:
                j = row * 4 + e[k]
                terms = [x.s.at[slot, j], x.d.at[slot, j]]
                if kind == "y":
                    arrive(x.rb.at[lax.rem(r, INBOX), e[k]], x.rr.at[lax.rem(r, INBOX), e[k]])
                    terms.append(x.rb.at[lax.rem(r, INBOX), e[k]])
                if inner:
                    arrive(x.rb.at[lax.rem(r, INBOX), base + e[k]], x.rr.at[lax.rem(r, INBOX), base + e[k]])
                    terms.append(x.rb.at[lax.rem(r, INBOX), base + e[k]])
                add(x, x.s.at[slot, j], *terms)
                along(x, r, slot, row, k, base)

    def outer(x, kind, r):
        if kind == "z":
            ready(x, r, lax.rem(r, SLOTS))
            granted(r, x.y_free)

        @pl.when(corner)
        def _():
            granted(r, x.on_free)
            onto(x, kind, r, (0, 1, 2), False)

    def inner(x, kind, r):
        @pl.when(mid)
        def _():
            granted(r, x.on_free)
            onto(x, kind, r, (0, 1), True)

    def last(x, kind, r):
        @pl.when(mid)
        def _():
            granted(r, x.back_free)
            onto(x, kind, r, (2,), True)

    def cross(x, kind, r):
        slot = lax.rem(r, SLOTS)
        j = (1 - y) * 4 + z
        ends(x, r, (1 - y) * 5)(lambda *got: add(x, x.s.at[slot, j], x.s.at[slot, j], x.d.at[slot, j], *got))
        send(x.s.at[slot, j], x.rb.at[lax.rem(r, INBOX), 10], x.ss.at[slot], x.rr.at[lax.rem(r, INBOX), 10], across).start()

    def share(x, kind, r, src, j, to_y, to_z):
        dst = blocks(x, x.out, r, j, c)
        if to_y:
            send(src, dst, x.ay.at[r], x.ar.at[r, j], across).start()
        if to_z:

            @pl.when(z < 3)
            def _():
                send(src, dst, x.az.at[r], x.ar.at[r, j], me + 2).start()

            @pl.when(z > 0)
            def _():
                send(src, dst, x.az.at[r], x.ar.at[r, j], me - 2).start()

        send(src, dst, x.ad, x.adr, partner).start()

    def step(x, kind, r):
        slot, at = lax.rem(r, SLOTS), lax.rem(r, LOADS)
        over = z if kind == "y" else 10
        arrive(x.rb.at[lax.rem(r, INBOX), over], x.rr.at[lax.rem(r, INBOX), over])
        base = 4 if kind == "y" else y * 5
        ends(x, r, base)(lambda *got: add(x, x.gb, x.s.at[slot, own], x.d.at[slot, own], x.rb.at[lax.rem(r, INBOX), over], *got))
        layer, rows, cols = piece(x.which, r)
        pltpu.make_async_copy(x.w.at[layer, own, c, rows, cols], x.wl.at[at], x.mo.at[at, 0]).wait()
        pltpu.make_async_copy(mine(x, x.m, r), x.ml.at[at], x.mo.at[at, 1]).wait()
        pltpu.make_async_copy(mine(x, x.v, r), x.vl.at[at], x.mo.at[at, 2]).wait()

        m, v = new_moments(x.ml[at], x.vl[at], x.gb[...].astype(jnp.float32))
        x.ml[at] = m
        x.vl[at] = v
        layer, rows, cols = piece(x.which, r)
        new, place = new_weight(x.wl[at].astype(jnp.float32), m, v), blocks(x, x.out, r, own, c)
        if HELD[x.which]:
            x.out[layer, own, c, rows, cols] = new
            share(x, kind, r, place, own, True, True)
        else:
            x.wb[r] = new
            share(x, kind, r, x.wb.at[r], own, True, True)
            pltpu.make_async_copy(x.wb.at[r], place, x.lo).start()
        for one in written(x, r, at):
            one.start()

        pl.when(r < ROUNDS - SLOTS)(lambda: grant(x.free, partner))

        @pl.when(r < ROUNDS - INBOX)
        def _():
            grant(x.y_free, across)

            @pl.when(mid)
            def _():
                grant(x.on_free, onward)
                grant(x.on_free, 2 * me - onward)

            @pl.when(corner)
            def _():
                grant(x.back_free, onward)

    def came(x, r, j):
        arrive(blocks(x, x.out, r, j, c), x.ar.at[r, j])
        return blocks(x, x.out, r, j, c)

    def pass0(x, kind, r):
        j = (1 - y) * 4 + z
        share(x, kind, r, came(x, r, j), j, False, True)

    def passes(x, kind, r, ks, inner):
        for row in (y,) if kind == "y" else (y, 1 - y):
            for k in ks:
                j = row * 4 + f[k]
                src = came(x, r, j)
                if inner:
                    send(src, src, x.az.at[r], x.ar.at[r, j], f_to[k]).start()
                share(x, kind, r, src, j, kind == "y", False)

    def hop1(x, kind, r):
        pl.when(mid)(lambda: passes(x, kind, r, (0, 1), True))
        pl.when(corner)(lambda: passes(x, kind, r, (0,), False))

    def hop2(x, kind, r):
        pl.when(mid)(lambda: passes(x, kind, r, (2,), True))
        pl.when(corner)(lambda: passes(x, kind, r, (1,), False))

    def hop3(x, kind, r):
        pl.when(corner)(lambda: passes(x, kind, r, (2,), False))

    def over(x, kind, r):
        for col in (z, *f):
            j = (1 - y) * 4 + col
            share(x, kind, r, came(x, r, j), j, False, False)

    stages = {one.__name__: one for one in (fetch, moments, first, outer, inner, last, cross, step, pass0, hop1, hop2, hop3, over)}

    barrier = pltpu.get_barrier_semaphore()
    pl.semaphore_signal(barrier, inc=1, device_id=(rep, partner), device_id_type=MESH)
    pl.semaphore_signal(barrier, inc=1, device_id=(rep, across), device_id_type=MESH)

    @pl.when(z < 3)
    def _():
        pl.semaphore_signal(barrier, inc=1, device_id=(rep, me + 2), device_id_type=MESH)

    @pl.when(z > 0)
    def _():
        pl.semaphore_signal(barrier, inc=1, device_id=(rep, me - 2), device_id_type=MESH)

    @pl.when(mid)
    def _():
        pl.semaphore_wait(barrier, 4)

    @pl.when(corner)
    def _():
        pl.semaphore_wait(barrier, 3)

    def turn(i, carry):
        for sub in range(3):
            for name in ORDER:
                for kind in ("y", "z"):
                    lag = LAGS[kind].get(name)
                    if lag is None:
                        continue
                    x = weights[(sub - lag) % 3]
                    r = i + (sub - lag) // 3
                    ok = (r >= 0) & (r < ROUNDS)
                    some, is_z = kinds(x.which, r, name in GATHER)
                    if name in ("fetch", "moments"):
                        if kind == "z":
                            continue
                    elif kind not in some:
                        continue
                    elif is_z is not None:
                        ok = ok & (is_z if kind == "z" else jnp.logical_not(is_z))
                    pl.when(ok)(functools.partial(stages[name], x, kind, r))
        return carry

    longest = max(max(kind.values()) for kind in LAGS.values())
    lax.fori_loop(0, ROUNDS + (longest + 2) // 3, turn, 0)

    for x in weights:
        for slot in range(SLOTS):
            left(x.s.at[slot, pl.ds(0, 7)], x.ss.at[slot])
        def gathered(r, carry):
            some, is_z = kinds(x.which, r, True)
            for kind in some:

                def sent():
                    left(x.s.at[0, pl.ds(0, 4 if kind == "y" else 1)], x.ay.at[r])
                    pl.when(mid)(lambda: left(x.s.at[pl.ds(0, 1 if kind == "y" else 2), pl.ds(0, 5)], x.az.at[r]))
                    pl.when(corner)(lambda: left(x.s.at[0, pl.ds(0, 1 if kind == "y" else 2)], x.az.at[r]))

                pl.when(True if is_z is None else is_z if kind == "z" else jnp.logical_not(is_z))(sent)
            return carry

        lax.fori_loop(0, ROUNDS, gathered, 0)
        left(x.out.at[:, :, 0], x.ds)
        left(x.out.at[:, :, 0], x.ad)
        arrive(x.out.at[:, :, 0], x.adr)
        if not HELD[x.which]:
            arrive(x.wb, x.lo)
        for r in range(ROUNDS - LOADS, ROUNDS):
            for one in written(x, jnp.int32(r), r % LOADS):
                one.wait()


def solution(mesh):
    def step(*arrays):
        terms, weights, m, v = (arrays[i : i + 3] for i in (0, 3, 6, 9))

        def cut(one):
            rows, cols = one.shape[-2:]
            return one.reshape(2, 8, 2, rows // 16, cols)

        wide = [cut(one) for one in weights]
        outs = pl.pallas_call(
            kernel,
            out_shape=[*((pltpu.VMEM if held else jax.ShapeDtypeStruct)(one.shape, one.dtype) for held, one in zip(HELD, wide, strict=True)), *(pltpu.HBM(one.shape, one.dtype) for one in (*m, *v))],
            in_specs=[ANY] * 12,
            out_specs=[pl.BlockSpec(memory_space=pltpu.VMEM) if held else ANY for held in HELD] + [ANY] * 6,
            scratch_shapes=[one for i in range(3) for one in scratch(i)],
            compiler_params=pltpu.CompilerParams(collective_id=0, has_side_effects=True, vmem_limit_bytes=16 * 2**20),
            name="sum_step_gather",
        )(*(pltpu.with_memory_space_constraint(one, pltpu.HBM) for one in (*(cut(t[0]) for t in terms), *wide, *m, *v)))
        whole = [one.reshape(w.shape) for one, w in zip(outs[:3], weights, strict=True)]
        return (*whole, *outs[3:])

    all_of, cut = P(None, None, None), P(None, "dp", None)
    return jax.shard_map(
        step,
        mesh=mesh,
        in_specs=(P(("rep", "dp"), None, None, None),) * 3 + (all_of,) * 3 + (cut,) * 6,
        out_specs=(P("rep", None, None),) * 3 + (P("rep", "dp", None),) * 6,
        check_vma=False,
    )
```

```python
import functools

import jax
import jax.numpy as jnp
from jax import lax
from jax.experimental import pallas as pl
from jax.experimental.pallas import tpu as pltpu
from jax.sharding import PartitionSpec as P

MESH = pl.DeviceIdType.MESH
ANY = pl.BlockSpec(memory_space=pl.ANY)
ROUNDS = 32
SLOTS = 5
INBOX = 5
HELD = (False, False, False)
RING = 4
LOADS = 2
NAMES = ("gate", "up", "down")
ALONE = 6


def kinds(which, r, gather):
    among = r >= ALONE if not gather else r < ROUNDS - ALONE
    if which == 0:
        return ("y",), None
    if which == 1:
        return ("y", "z"), among | (lax.rem(r + ROUNDS, 2) == 1)
    return ("y", "z"), among & (lax.rem(r + ROUNDS, 4) == 3)


LAGS = {
    "y": {"fetch": 0, "first": 2, "outer": 4, "inner": 6, "last": 8, "moments": 7, "step": 10, "hop1": 12, "hop2": 14, "hop3": 16, "over": 18},
    "z": {"fetch": 0, "outer": 2, "inner": 4, "last": 6, "cross": 8, "moments": 7, "step": 10, "pass0": 12, "hop1": 14, "hop2": 16, "hop3": 18},
}
ORDER = ("fetch", "moments", "first", "outer", "inner", "last", "cross", "step", "pass0", "hop1", "hop2", "hop3", "over")
KEYS = ("s", "d", "rb", "wb", "gb", "wl", "ml", "vl", "ld", "dr", "ds", "ss", "rr", "ar", "ad", "ay", "az", "adr", "mo", "mw", "lo", "free", "y_free", "on_free", "back_free")


def new_moments(m, v, g):
    return 0.9 * m + 0.1 * g, 0.95 * v + 0.05 * g * g


def new_weight(w, m, v):
    return (w - 0.02 * (m * lax.rsqrt(v + 1e-8) + 0.1 * w)).astype(jnp.bfloat16)


def piece(which, r):
    rows, cols = shape_of(which)
    across = (1024 if which == 2 else 3584) // cols
    layer, q = r // (ROUNDS // 2), lax.rem(r, ROUNDS // 2)
    return layer, pl.ds(pl.multiple_of(q // across * rows, rows), rows), pl.ds(pl.multiple_of(lax.rem(q, across) * cols, cols), cols)


def shape_of(which):
    return (112, 4096 // ROUNDS) if which == 2 else (16, 28672 // ROUNDS)


def scratch(which):
    rows, cols = shape_of(which)
    bf, f32, dma = jnp.bfloat16, jnp.float32, pltpu.SemaphoreType.DMA
    return (
        pltpu.VMEM((SLOTS, 8, rows, cols), bf),
        pltpu.VMEM((SLOTS, 8, rows, cols), bf),
        pltpu.VMEM((INBOX, 9 if which == 0 else 11, rows, cols), bf),
        pltpu.VMEM((1 if HELD[which] else ROUNDS, rows, cols), bf),
        pltpu.VMEM((rows, cols), bf),
        pltpu.VMEM((LOADS, rows, cols), bf),
        pltpu.VMEM((LOADS, rows, cols), f32),
        pltpu.VMEM((LOADS, rows, cols), f32),
        dma((SLOTS,)),
        dma((SLOTS,)),
        dma,
        dma((SLOTS,)),
        dma((INBOX, 11)),
        dma((ROUNDS, 8)),
        dma,
        dma((ROUNDS,)),
        dma((ROUNDS,)),
        dma,
        dma((LOADS, 3)),
        dma((LOADS, 2)),
        dma,
        *([pltpu.SemaphoreType.REGULAR] * 4),
    )


class Weight:
    pass


GATHER = ("pass0", "hop1", "hop2", "hop3", "over")


def kernel(*refs):
    rep, me = lax.axis_index("rep"), lax.axis_index("dp")
    y, z, c = me // 8, lax.rem(me // 2, 4), lax.rem(me, 2)
    own = me // 2
    partner, across = me + 1 - 2 * c, me + 8 - 16 * y
    mid = (z > 0) & (z < 3)
    corner = (z == 0) | (z == 3)
    low = 1 - z // 2
    odd = lax.rem(z, 2)
    onward = me + 4 * low - 2
    e = (3 * low, 1 + low, low * (1 - z) + (1 - low) * (5 - z))
    e_to = (onward, onward, me + 2 - 4 * odd)
    e_slot = (e[0], e[1] + z // 2 * (1 - odd) * (4 - e[1]), e[2] + odd * (4 - e[2]))
    f = (z + 1 - 2 * odd, 2 - z // 2, 3 * low)
    f_to = (onward, me + 2 - 4 * low, me + 2 - 4 * low)

    inputs, outputs, rest = refs[:12], refs[12:21], refs[21:]
    weights = []
    for i in range(3):
        x = Weight()
        x.which = i
        x.g, x.w, x.m, x.v = inputs[i], inputs[3 + i], inputs[6 + i], inputs[9 + i]
        x.out, x.mout, x.vout = outputs[i], outputs[3 + i], outputs[6 + i]
        for key, ref in zip(KEYS, rest[i * len(KEYS) : (i + 1) * len(KEYS)], strict=True):
            setattr(x, key, ref)
        weights.append(x)

    def send(src, dst, sent, got, to):
        return pltpu.make_async_remote_copy(src_ref=src, dst_ref=dst, send_sem=sent, recv_sem=got, device_id=(rep, to), device_id_type=MESH)

    def arrive(ref, sem):
        send(ref, ref, sem, sem, partner).wait_recv()

    def left(ref, sem):
        send(ref, ref, sem, sem, partner).wait_send()

    def blocks(x, ref, r, j, core):
        layer, rows, cols = piece(x.which, r)
        return ref.at[layer, j, core, rows, cols]

    def mine(x, ref, r):
        layer, rows, cols = piece(x.which, r)
        return ref.at[layer, rows, cols]

    def add(x, dst, *terms):
        total = terms[0][...].astype(jnp.float32)
        for term in terms[1:]:
            total += term[...].astype(jnp.float32)
        dst[...] = total.astype(jnp.bfloat16)

    def ends(x, r, base):
        def when(then):
            @pl.when(mid)
            def _():
                arrive(x.rb.at[lax.rem(r, INBOX), base + z], x.rr.at[lax.rem(r, INBOX), base + z])
                arrive(x.rb.at[lax.rem(r, INBOX), base + 4], x.rr.at[lax.rem(r, INBOX), base + 4])
                then(x.rb.at[lax.rem(r, INBOX), base + z], x.rb.at[lax.rem(r, INBOX), base + 4])

            @pl.when(corner)
            def _():
                at = base + 4 - z // 3
                arrive(x.rb.at[lax.rem(r, INBOX), at], x.rr.at[lax.rem(r, INBOX), at])
                then(x.rb.at[lax.rem(r, INBOX), at])

        return when

    def fetch(x, kind, r):
        slot = lax.rem(r, SLOTS)

        @pl.when(r >= SLOTS)
        def _():
            left(x.s.at[slot, pl.ds(0, 7)], x.ss.at[slot])
            pl.semaphore_wait(x.free, 1)

        pltpu.make_async_copy(blocks(x, x.g, r, slice(None), c), x.s.at[slot], x.ld.at[slot]).start()
        send(blocks(x, x.g, r, slice(None), 1 - c), x.d.at[slot], x.ds, x.dr.at[slot], partner).start()

    def written(x, r, slot):
        return (
            pltpu.make_async_copy(x.ml.at[slot], mine(x, x.mout, r), x.mw.at[slot, 0]),
            pltpu.make_async_copy(x.vl.at[slot], mine(x, x.vout, r), x.mw.at[slot, 1]),
        )

    def moments(x, kind, r):
        slot = lax.rem(r, LOADS)
        layer, rows, cols = piece(x.which, r)

        @pl.when(r >= LOADS)
        def _():
            for one in written(x, r, slot):
                one.wait()

        pltpu.make_async_copy(x.w.at[layer, own, c, rows, cols], x.wl.at[slot], x.mo.at[slot, 0]).start()
        pltpu.make_async_copy(mine(x, x.m, r), x.ml.at[slot], x.mo.at[slot, 1]).start()
        pltpu.make_async_copy(mine(x, x.v, r), x.vl.at[slot], x.mo.at[slot, 2]).start()

    def along(x, r, slot, row, k, base, *terms):
        j = row * 4 + e[k]
        to = base + e_slot[k]
        send(x.s.at[slot, j], x.rb.at[lax.rem(r, INBOX), to], x.ss.at[slot], x.rr.at[lax.rem(r, INBOX), to], e_to[k]).start()

    def ready(x, r, slot):
        pltpu.make_async_copy(blocks(x, x.g, r, slice(None), c), x.s.at[slot], x.ld.at[slot]).wait()
        arrive(x.d.at[slot], x.dr.at[slot])

    def granted(r, free):
        pl.when(r >= INBOX)(lambda: pl.semaphore_wait(free, 1))

    def grant(free, to):
        pl.semaphore_signal(free, inc=1, device_id=(rep, to), device_id_type=MESH)

    def first(x, kind, r):
        slot = lax.rem(r, SLOTS)
        ready(x, r, slot)
        granted(r, x.y_free)
        for col in (*e, z):
            j = (1 - y) * 4 + col
            add(x, x.s.at[slot, j], x.s.at[slot, j], x.d.at[slot, j])
            send(x.s.at[slot, j], x.rb.at[lax.rem(r, INBOX), col], x.ss.at[slot], x.rr.at[lax.rem(r, INBOX), col], across).start()

    def onto(x, kind, r, ks, inner):
        slot = lax.rem(r, SLOTS)
        for row in (y,) if kind == "y" else (1 - y, y):
            base = 4 if kind == "y" else row * 5
            for k in ks:
                j = row * 4 + e[k]
                terms = [x.s.at[slot, j], x.d.at[slot, j]]
                if kind == "y":
                    arrive(x.rb.at[lax.rem(r, INBOX), e[k]], x.rr.at[lax.rem(r, INBOX), e[k]])
                    terms.append(x.rb.at[lax.rem(r, INBOX), e[k]])
                if inner:
                    arrive(x.rb.at[lax.rem(r, INBOX), base + e[k]], x.rr.at[lax.rem(r, INBOX), base + e[k]])
                    terms.append(x.rb.at[lax.rem(r, INBOX), base + e[k]])
                add(x, x.s.at[slot, j], *terms)
                along(x, r, slot, row, k, base)

    def outer(x, kind, r):
        if kind == "z":
            ready(x, r, lax.rem(r, SLOTS))
            granted(r, x.y_free)

        @pl.when(corner)
        def _():
            granted(r, x.on_free)
            onto(x, kind, r, (0, 1, 2), False)

    def inner(x, kind, r):
        @pl.when(mid)
        def _():
            granted(r, x.on_free)
            onto(x, kind, r, (0, 1), True)

    def last(x, kind, r):
        @pl.when(mid)
        def _():
            granted(r, x.back_free)
            onto(x, kind, r, (2,), True)

    def cross(x, kind, r):
        slot = lax.rem(r, SLOTS)
        j = (1 - y) * 4 + z
        ends(x, r, (1 - y) * 5)(lambda *got: add(x, x.s.at[slot, j], x.s.at[slot, j], x.d.at[slot, j], *got))
        send(x.s.at[slot, j], x.rb.at[lax.rem(r, INBOX), 10], x.ss.at[slot], x.rr.at[lax.rem(r, INBOX), 10], across).start()

    def share(x, kind, r, src, j, to_y, to_z):
        dst = blocks(x, x.out, r, j, c)
        if to_y:
            send(src, dst, x.ay.at[r], x.ar.at[r, j], across).start()
        if to_z:

            @pl.when(z < 3)
            def _():
                send(src, dst, x.az.at[r], x.ar.at[r, j], me + 2).start()

            @pl.when(z > 0)
            def _():
                send(src, dst, x.az.at[r], x.ar.at[r, j], me - 2).start()

        send(src, dst, x.ad, x.adr, partner).start()

    def step(x, kind, r):
        slot, at = lax.rem(r, SLOTS), lax.rem(r, LOADS)
        over = z if kind == "y" else 10
        arrive(x.rb.at[lax.rem(r, INBOX), over], x.rr.at[lax.rem(r, INBOX), over])
        base = 4 if kind == "y" else y * 5
        ends(x, r, base)(lambda *got: add(x, x.gb, x.s.at[slot, own], x.d.at[slot, own], x.rb.at[lax.rem(r, INBOX), over], *got))
        layer, rows, cols = piece(x.which, r)
        pltpu.make_async_copy(x.w.at[layer, own, c, rows, cols], x.wl.at[at], x.mo.at[at, 0]).wait()
        pltpu.make_async_copy(mine(x, x.m, r), x.ml.at[at], x.mo.at[at, 1]).wait()
        pltpu.make_async_copy(mine(x, x.v, r), x.vl.at[at], x.mo.at[at, 2]).wait()

        m, v = new_moments(x.ml[at], x.vl[at], x.gb[...].astype(jnp.float32))
        x.ml[at] = m
        x.vl[at] = v
        layer, rows, cols = piece(x.which, r)
        new, place = new_weight(x.wl[at].astype(jnp.float32), m, v), blocks(x, x.out, r, own, c)
        if HELD[x.which]:
            x.out[layer, own, c, rows, cols] = new
            share(x, kind, r, place, own, True, True)
        else:
            x.wb[r] = new
            share(x, kind, r, x.wb.at[r], own, True, True)
            pltpu.make_async_copy(x.wb.at[r], place, x.lo).start()
        for one in written(x, r, at):
            one.start()

        pl.when(r < ROUNDS - SLOTS)(lambda: grant(x.free, partner))

        @pl.when(r < ROUNDS - INBOX)
        def _():
            grant(x.y_free, across)

            @pl.when(mid)
            def _():
                grant(x.on_free, onward)
                grant(x.on_free, 2 * me - onward)

            @pl.when(corner)
            def _():
                grant(x.back_free, onward)

    def came(x, r, j):
        arrive(blocks(x, x.out, r, j, c), x.ar.at[r, j])
        return blocks(x, x.out, r, j, c)

    def pass0(x, kind, r):
        j = (1 - y) * 4 + z
        share(x, kind, r, came(x, r, j), j, False, True)

    def passes(x, kind, r, ks, inner):
        for row in (y,) if kind == "y" else (y, 1 - y):
            for k in ks:
                j = row * 4 + f[k]
                src = came(x, r, j)
                if inner:
                    send(src, src, x.az.at[r], x.ar.at[r, j], f_to[k]).start()
                share(x, kind, r, src, j, kind == "y", False)

    def hop1(x, kind, r):
        pl.when(mid)(lambda: passes(x, kind, r, (0, 1), True))
        pl.when(corner)(lambda: passes(x, kind, r, (0,), False))

    def hop2(x, kind, r):
        pl.when(mid)(lambda: passes(x, kind, r, (2,), True))
        pl.when(corner)(lambda: passes(x, kind, r, (1,), False))

    def hop3(x, kind, r):
        pl.when(corner)(lambda: passes(x, kind, r, (2,), False))

    def over(x, kind, r):
        for col in (z, *f):
            j = (1 - y) * 4 + col
            share(x, kind, r, came(x, r, j), j, False, False)

    stages = {one.__name__: one for one in (fetch, moments, first, outer, inner, last, cross, step, pass0, hop1, hop2, hop3, over)}

    barrier = pltpu.get_barrier_semaphore()
    pl.semaphore_signal(barrier, inc=1, device_id=(rep, partner), device_id_type=MESH)
    pl.semaphore_signal(barrier, inc=1, device_id=(rep, across), device_id_type=MESH)

    @pl.when(z < 3)
    def _():
        pl.semaphore_signal(barrier, inc=1, device_id=(rep, me + 2), device_id_type=MESH)

    @pl.when(z > 0)
    def _():
        pl.semaphore_signal(barrier, inc=1, device_id=(rep, me - 2), device_id_type=MESH)

    @pl.when(mid)
    def _():
        pl.semaphore_wait(barrier, 4)

    @pl.when(corner)
    def _():
        pl.semaphore_wait(barrier, 3)

    def turn(i, carry):
        for sub in range(3):
            for name in ORDER:
                for kind in ("y", "z"):
                    lag = LAGS[kind].get(name)
                    if lag is None:
                        continue
                    x = weights[(sub - lag) % 3]
                    r = i + (sub - lag) // 3
                    ok = (r >= 0) & (r < ROUNDS)
                    some, is_z = kinds(x.which, r, name in GATHER)
                    if name in ("fetch", "moments"):
                        if kind == "z":
                            continue
                    elif kind not in some:
                        continue
                    elif is_z is not None:
                        ok = ok & (is_z if kind == "z" else jnp.logical_not(is_z))
                    pl.when(ok)(functools.partial(stages[name], x, kind, r))
        return carry

    longest = max(max(kind.values()) for kind in LAGS.values())
    lax.fori_loop(0, ROUNDS + (longest + 2) // 3, turn, 0)

    for x in weights:
        for slot in range(SLOTS):
            left(x.s.at[slot, pl.ds(0, 7)], x.ss.at[slot])
        def gathered(r, carry):
            some, is_z = kinds(x.which, r, True)
            for kind in some:

                def sent():
                    left(x.s.at[0, pl.ds(0, 4 if kind == "y" else 1)], x.ay.at[r])
                    pl.when(mid)(lambda: left(x.s.at[pl.ds(0, 1 if kind == "y" else 2), pl.ds(0, 5)], x.az.at[r]))
                    pl.when(corner)(lambda: left(x.s.at[0, pl.ds(0, 1 if kind == "y" else 2)], x.az.at[r]))

                pl.when(True if is_z is None else is_z if kind == "z" else jnp.logical_not(is_z))(sent)
            return carry

        lax.fori_loop(0, ROUNDS, gathered, 0)
        left(x.out.at[:, :, 0], x.ds)
        left(x.out.at[:, :, 0], x.ad)
        arrive(x.out.at[:, :, 0], x.adr)
        if not HELD[x.which]:
            arrive(x.wb, x.lo)
        for r in range(ROUNDS - LOADS, ROUNDS):
            for one in written(x, jnp.int32(r), r % LOADS):
                one.wait()


def finish(*refs):
    ins, outs, stages, ring = refs[:9], refs[9:18], refs[18:24], refs[24]
    sent, loaded, stored, taken, given = refs[25:]
    puts = []
    for i in range(2):
        rows = outs[i].shape[1] // 4
        for k in range(8):
            part = (k // 4, pl.ds(k % 4 * rows, rows))
            puts.append(pltpu.make_async_copy(ins[i].at[part], outs[i].at[part], sent.at[i, k]))
    loads = [pltpu.make_async_copy(ins[3 + i], stages[i], loaded.at[i]) for i in range(6)]
    stores = [pltpu.make_async_copy(stages[i], outs[3 + i], stored.at[i]) for i in range(6)]
    takes, gives = [], []
    rows = ring.shape[1]
    for k in range(2 * (3584 // rows)):
        part, slot = (k // (3584 // rows), pl.ds(k % (3584 // rows) * rows, rows)), k % RING
        takes.append(pltpu.make_async_copy(ins[2].at[part], ring.at[slot], taken.at[slot]))
        gives.append(pltpu.make_async_copy(ring.at[slot], outs[2].at[part], given.at[slot]))
    for one in (*takes[:RING], *loads[:2], *puts, *loads[2:]):
        one.start()
    for k, (take, give) in enumerate(zip(takes, gives, strict=True)):
        take.wait()
        give.start()
        if k >= 1 and k - 1 + RING < len(takes):
            gives[k - 1].wait()
            takes[k - 1 + RING].start()
        if k % 2 and k // 2 < 6:
            loads[k // 2].wait()
            stores[k // 2].start()
    for one in (*gives[-RING:], *puts, *stores):
        one.wait()


def solution(mesh):
    def step(*arrays):
        terms, weights, m, v = (arrays[i : i + 3] for i in (0, 3, 6, 9))

        def cut(one):
            rows, cols = one.shape[-2:]
            return one.reshape(2, 8, 2, rows // 16, cols)

        wide = [cut(one) for one in weights]
        outs = pl.pallas_call(
            kernel,
            out_shape=[*((pltpu.VMEM if held else jax.ShapeDtypeStruct)(one.shape, one.dtype) for held, one in zip(HELD, wide, strict=True)), *(pltpu.HBM(one.shape, one.dtype) for one in (*m, *v))],
            in_specs=[ANY] * 12,
            out_specs=[pl.BlockSpec(memory_space=pltpu.VMEM) if held else ANY for held in HELD] + [ANY] * 6,
            scratch_shapes=[one for i in range(3) for one in scratch(i)],
            compiler_params=pltpu.CompilerParams(collective_id=0, has_side_effects=True, vmem_limit_bytes=16 * 2**20),
            name="sum_step_gather",
        )(*(pltpu.with_memory_space_constraint(one, pltpu.HBM) for one in (*(cut(t[0]) for t in terms), *wide, *m, *v)))
        whole = [one.reshape(w.shape) for one, w in zip(outs[:3], weights, strict=True)]
        kept = [pltpu.with_memory_space_constraint(one, pltpu.HBM) for one in (whole[2], *outs[3:])]
        dma = pltpu.SemaphoreType.DMA
        return pl.pallas_call(
            finish,
            out_shape=[jax.ShapeDtypeStruct(one.shape, one.dtype) for one in (*whole[:2], *kept)],
            in_specs=[ANY] * 9,
            out_specs=[ANY] * 9,
            scratch_shapes=[*(pltpu.VMEM(one.shape, one.dtype) for one in kept[1:]), pltpu.VMEM((RING, 448, 1024), jnp.bfloat16), dma((2, 8)), dma((6,)), dma((6,)), dma((RING,)), dma((RING,))],
            compiler_params=pltpu.CompilerParams(vmem_limit_bytes=15 * 2**20),
            name="finish",
        )(*whole[:2], *kept)

    all_of, cut = P(None, None, None), P(None, "dp", None)
    return jax.shard_map(
        step,
        mesh=mesh,
        in_specs=(P(("rep", "dp"), None, None, None),) * 3 + (all_of,) * 3 + (cut,) * 6,
        out_specs=(P("rep", None, None),) * 3 + (P("rep", "dp", None),) * 6,
        check_vma=False,
    )
```

```python
import functools

import jax
import jax.numpy as jnp
from jax import lax
from jax.experimental import pallas as pl
from jax.experimental.pallas import tpu as pltpu
from jax.sharding import PartitionSpec as P

MESH = pl.DeviceIdType.MESH
ANY = pl.BlockSpec(memory_space=pl.ANY)
ROUNDS = 32
SLOTS = 5
INBOX = 5
HELD = (False, False, False)
RING = 5
LOADS = 2
NAMES = ("gate", "up", "down")
ALONE = 6


def kinds(which, r, gather):
    among = r >= ALONE if not gather else r < ROUNDS - ALONE
    if which == 0:
        return ("y",), None
    if which == 1:
        return ("y", "z"), among | (lax.rem(r + ROUNDS, 2) == 1)
    return ("y", "z"), among & (lax.rem(r + ROUNDS, 4) == 1)


LAGS = {
    "y": {"fetch": 0, "first": 2, "outer": 4, "inner": 6, "last": 8, "moments": 7, "step": 10, "hop1": 12, "hop2": 14, "hop3": 16, "over": 18},
    "z": {"fetch": 0, "outer": 2, "inner": 4, "last": 6, "cross": 8, "moments": 7, "step": 10, "pass0": 12, "hop1": 14, "hop2": 16, "hop3": 18},
}
ORDER = ("fetch", "moments", "first", "outer", "inner", "last", "cross", "step", "pass0", "hop1", "hop2", "hop3", "over")
KEYS = ("s", "d", "rb", "wb", "gb", "wl", "ml", "vl", "ld", "dr", "ds", "ss", "rr", "ar", "ad", "ay", "az", "adr", "mo", "mw", "lo", "free", "y_free", "on_free", "back_free")


def new_moments(m, v, g):
    return 0.9 * m + 0.1 * g, 0.95 * v + 0.05 * g * g


def new_weight(w, m, v):
    return (w - 0.02 * (m * lax.rsqrt(v + 1e-8) + 0.1 * w)).astype(jnp.bfloat16)


def piece(which, r):
    rows, cols = shape_of(which)
    across = (1024 if which == 2 else 3584) // cols
    layer, q = r // (ROUNDS // 2), lax.rem(r, ROUNDS // 2)
    return layer, pl.ds(pl.multiple_of(q // across * rows, rows), rows), pl.ds(pl.multiple_of(lax.rem(q, across) * cols, cols), cols)


def shape_of(which):
    return (112, 4096 // ROUNDS) if which == 2 else (16, 28672 // ROUNDS)


def scratch(which):
    rows, cols = shape_of(which)
    bf, f32, dma = jnp.bfloat16, jnp.float32, pltpu.SemaphoreType.DMA
    return (
        pltpu.VMEM((SLOTS, 8, rows, cols), bf),
        pltpu.VMEM((SLOTS, 8, rows, cols), bf),
        pltpu.VMEM((INBOX, 9 if which == 0 else 11, rows, cols), bf),
        pltpu.VMEM((1 if HELD[which] else ROUNDS, rows, cols), bf),
        pltpu.VMEM((rows, cols), bf),
        pltpu.VMEM((LOADS, rows, cols), bf),
        pltpu.VMEM((LOADS, rows, cols), f32),
        pltpu.VMEM((LOADS, rows, cols), f32),
        dma((SLOTS,)),
        dma((SLOTS,)),
        dma,
        dma((SLOTS,)),
        dma((INBOX, 11)),
        dma((ROUNDS, 8)),
        dma,
        dma((ROUNDS,)),
        dma((ROUNDS,)),
        dma,
        dma((LOADS, 3)),
        dma((LOADS, 2)),
        dma,
        *([pltpu.SemaphoreType.REGULAR] * 4),
    )


class Weight:
    pass


GATHER = ("pass0", "hop1", "hop2", "hop3", "over")


def kernel(*refs):
    rep, me = lax.axis_index("rep"), lax.axis_index("dp")
    y, z, c = me // 8, lax.rem(me // 2, 4), lax.rem(me, 2)
    own = me // 2
    partner, across = me + 1 - 2 * c, me + 8 - 16 * y
    mid = (z > 0) & (z < 3)
    corner = (z == 0) | (z == 3)
    low = 1 - z // 2
    odd = lax.rem(z, 2)
    onward = me + 4 * low - 2
    e = (3 * low, 1 + low, low * (1 - z) + (1 - low) * (5 - z))
    e_to = (onward, onward, me + 2 - 4 * odd)
    e_slot = (e[0], e[1] + z // 2 * (1 - odd) * (4 - e[1]), e[2] + odd * (4 - e[2]))
    f = (z + 1 - 2 * odd, 2 - z // 2, 3 * low)
    f_to = (onward, me + 2 - 4 * low, me + 2 - 4 * low)

    inputs, outputs, rest = refs[:12], refs[12:21], refs[21:]
    weights = []
    for i in range(3):
        x = Weight()
        x.which = i
        x.g, x.w, x.m, x.v = inputs[i], inputs[3 + i], inputs[6 + i], inputs[9 + i]
        x.out, x.mout, x.vout = outputs[i], outputs[3 + i], outputs[6 + i]
        for key, ref in zip(KEYS, rest[i * len(KEYS) : (i + 1) * len(KEYS)], strict=True):
            setattr(x, key, ref)
        weights.append(x)

    def send(src, dst, sent, got, to):
        return pltpu.make_async_remote_copy(src_ref=src, dst_ref=dst, send_sem=sent, recv_sem=got, device_id=(rep, to), device_id_type=MESH)

    def arrive(ref, sem):
        send(ref, ref, sem, sem, partner).wait_recv()

    def left(ref, sem):
        send(ref, ref, sem, sem, partner).wait_send()

    def blocks(x, ref, r, j, core):
        layer, rows, cols = piece(x.which, r)
        return ref.at[layer, j, core, rows, cols]

    def mine(x, ref, r):
        layer, rows, cols = piece(x.which, r)
        return ref.at[layer, rows, cols]

    def add(x, dst, *terms):
        total = terms[0][...].astype(jnp.float32)
        for term in terms[1:]:
            total += term[...].astype(jnp.float32)
        dst[...] = total.astype(jnp.bfloat16)

    def ends(x, r, base):
        def when(then):
            @pl.when(mid)
            def _():
                arrive(x.rb.at[lax.rem(r, INBOX), base + z], x.rr.at[lax.rem(r, INBOX), base + z])
                arrive(x.rb.at[lax.rem(r, INBOX), base + 4], x.rr.at[lax.rem(r, INBOX), base + 4])
                then(x.rb.at[lax.rem(r, INBOX), base + z], x.rb.at[lax.rem(r, INBOX), base + 4])

            @pl.when(corner)
            def _():
                at = base + 4 - z // 3
                arrive(x.rb.at[lax.rem(r, INBOX), at], x.rr.at[lax.rem(r, INBOX), at])
                then(x.rb.at[lax.rem(r, INBOX), at])

        return when

    def fetch(x, kind, r):
        slot = lax.rem(r, SLOTS)

        @pl.when(r >= SLOTS)
        def _():
            left(x.s.at[slot, pl.ds(0, 7)], x.ss.at[slot])
            pl.semaphore_wait(x.free, 1)

        pltpu.make_async_copy(blocks(x, x.g, r, slice(None), c), x.s.at[slot], x.ld.at[slot]).start()
        send(blocks(x, x.g, r, slice(None), 1 - c), x.d.at[slot], x.ds, x.dr.at[slot], partner).start()

    def written(x, r, slot):
        return (
            pltpu.make_async_copy(x.ml.at[slot], mine(x, x.mout, r), x.mw.at[slot, 0]),
            pltpu.make_async_copy(x.vl.at[slot], mine(x, x.vout, r), x.mw.at[slot, 1]),
        )

    def moments(x, kind, r):
        slot = lax.rem(r, LOADS)
        layer, rows, cols = piece(x.which, r)

        @pl.when(r >= LOADS)
        def _():
            for one in written(x, r, slot):
                one.wait()

        pltpu.make_async_copy(x.w.at[layer, own, c, rows, cols], x.wl.at[slot], x.mo.at[slot, 0]).start()
        pltpu.make_async_copy(mine(x, x.m, r), x.ml.at[slot], x.mo.at[slot, 1]).start()
        pltpu.make_async_copy(mine(x, x.v, r), x.vl.at[slot], x.mo.at[slot, 2]).start()

    def along(x, r, slot, row, k, base, *terms):
        j = row * 4 + e[k]
        to = base + e_slot[k]
        send(x.s.at[slot, j], x.rb.at[lax.rem(r, INBOX), to], x.ss.at[slot], x.rr.at[lax.rem(r, INBOX), to], e_to[k]).start()

    def ready(x, r, slot):
        pltpu.make_async_copy(blocks(x, x.g, r, slice(None), c), x.s.at[slot], x.ld.at[slot]).wait()
        arrive(x.d.at[slot], x.dr.at[slot])

    def granted(r, free):
        pl.when(r >= INBOX)(lambda: pl.semaphore_wait(free, 1))

    def grant(free, to):
        pl.semaphore_signal(free, inc=1, device_id=(rep, to), device_id_type=MESH)

    def first(x, kind, r):
        slot = lax.rem(r, SLOTS)
        ready(x, r, slot)
        granted(r, x.y_free)
        for col in (*e, z):
            j = (1 - y) * 4 + col
            add(x, x.s.at[slot, j], x.s.at[slot, j], x.d.at[slot, j])
            send(x.s.at[slot, j], x.rb.at[lax.rem(r, INBOX), col], x.ss.at[slot], x.rr.at[lax.rem(r, INBOX), col], across).start()

    def onto(x, kind, r, ks, inner):
        slot = lax.rem(r, SLOTS)
        for row in (y,) if kind == "y" else (1 - y, y):
            base = 4 if kind == "y" else row * 5
            for k in ks:
                j = row * 4 + e[k]
                terms = [x.s.at[slot, j], x.d.at[slot, j]]
                if kind == "y":
                    arrive(x.rb.at[lax.rem(r, INBOX), e[k]], x.rr.at[lax.rem(r, INBOX), e[k]])
                    terms.append(x.rb.at[lax.rem(r, INBOX), e[k]])
                if inner:
                    arrive(x.rb.at[lax.rem(r, INBOX), base + e[k]], x.rr.at[lax.rem(r, INBOX), base + e[k]])
                    terms.append(x.rb.at[lax.rem(r, INBOX), base + e[k]])
                add(x, x.s.at[slot, j], *terms)
                along(x, r, slot, row, k, base)

    def outer(x, kind, r):
        if kind == "z":
            ready(x, r, lax.rem(r, SLOTS))
            granted(r, x.y_free)

        @pl.when(corner)
        def _():
            granted(r, x.on_free)
            onto(x, kind, r, (0, 1, 2), False)

    def inner(x, kind, r):
        @pl.when(mid)
        def _():
            granted(r, x.on_free)
            onto(x, kind, r, (0, 1), True)

    def last(x, kind, r):
        @pl.when(mid)
        def _():
            granted(r, x.back_free)
            onto(x, kind, r, (2,), True)

    def cross(x, kind, r):
        slot = lax.rem(r, SLOTS)
        j = (1 - y) * 4 + z
        ends(x, r, (1 - y) * 5)(lambda *got: add(x, x.s.at[slot, j], x.s.at[slot, j], x.d.at[slot, j], *got))
        send(x.s.at[slot, j], x.rb.at[lax.rem(r, INBOX), 10], x.ss.at[slot], x.rr.at[lax.rem(r, INBOX), 10], across).start()

    def share(x, kind, r, src, j, to_y, to_z):
        dst = blocks(x, x.out, r, j, c)
        if to_y:
            send(src, dst, x.ay.at[r], x.ar.at[r, j], across).start()
        if to_z:

            @pl.when(z < 3)
            def _():
                send(src, dst, x.az.at[r], x.ar.at[r, j], me + 2).start()

            @pl.when(z > 0)
            def _():
                send(src, dst, x.az.at[r], x.ar.at[r, j], me - 2).start()

        send(src, dst, x.ad, x.adr, partner).start()

    def step(x, kind, r):
        slot, at = lax.rem(r, SLOTS), lax.rem(r, LOADS)
        over = z if kind == "y" else 10
        arrive(x.rb.at[lax.rem(r, INBOX), over], x.rr.at[lax.rem(r, INBOX), over])
        base = 4 if kind == "y" else y * 5
        ends(x, r, base)(lambda *got: add(x, x.gb, x.s.at[slot, own], x.d.at[slot, own], x.rb.at[lax.rem(r, INBOX), over], *got))
        layer, rows, cols = piece(x.which, r)
        pltpu.make_async_copy(x.w.at[layer, own, c, rows, cols], x.wl.at[at], x.mo.at[at, 0]).wait()
        pltpu.make_async_copy(mine(x, x.m, r), x.ml.at[at], x.mo.at[at, 1]).wait()
        pltpu.make_async_copy(mine(x, x.v, r), x.vl.at[at], x.mo.at[at, 2]).wait()

        m, v = new_moments(x.ml[at], x.vl[at], x.gb[...].astype(jnp.float32))
        x.ml[at] = m
        x.vl[at] = v
        layer, rows, cols = piece(x.which, r)
        new, place = new_weight(x.wl[at].astype(jnp.float32), m, v), blocks(x, x.out, r, own, c)
        if HELD[x.which]:
            x.out[layer, own, c, rows, cols] = new
            share(x, kind, r, place, own, True, True)
        else:
            x.wb[r] = new
            share(x, kind, r, x.wb.at[r], own, True, True)
            pltpu.make_async_copy(x.wb.at[r], place, x.lo).start()
        for one in written(x, r, at):
            one.start()

        pl.when(r < ROUNDS - SLOTS)(lambda: grant(x.free, partner))

        @pl.when(r < ROUNDS - INBOX)
        def _():
            grant(x.y_free, across)

            @pl.when(mid)
            def _():
                grant(x.on_free, onward)
                grant(x.on_free, 2 * me - onward)

            @pl.when(corner)
            def _():
                grant(x.back_free, onward)

    def came(x, r, j):
        arrive(blocks(x, x.out, r, j, c), x.ar.at[r, j])
        return blocks(x, x.out, r, j, c)

    def pass0(x, kind, r):
        j = (1 - y) * 4 + z
        share(x, kind, r, came(x, r, j), j, False, True)

    def passes(x, kind, r, ks, inner):
        for row in (y,) if kind == "y" else (y, 1 - y):
            for k in ks:
                j = row * 4 + f[k]
                src = came(x, r, j)
                if inner:
                    send(src, src, x.az.at[r], x.ar.at[r, j], f_to[k]).start()
                share(x, kind, r, src, j, kind == "y", False)

    def hop1(x, kind, r):
        pl.when(mid)(lambda: passes(x, kind, r, (0, 1), True))
        pl.when(corner)(lambda: passes(x, kind, r, (0,), False))

    def hop2(x, kind, r):
        pl.when(mid)(lambda: passes(x, kind, r, (2,), True))
        pl.when(corner)(lambda: passes(x, kind, r, (1,), False))

    def hop3(x, kind, r):
        pl.when(corner)(lambda: passes(x, kind, r, (2,), False))

    def over(x, kind, r):
        for col in (z, *f):
            j = (1 - y) * 4 + col
            share(x, kind, r, came(x, r, j), j, False, False)

    stages = {one.__name__: one for one in (fetch, moments, first, outer, inner, last, cross, step, pass0, hop1, hop2, hop3, over)}

    barrier = pltpu.get_barrier_semaphore()
    pl.semaphore_signal(barrier, inc=1, device_id=(rep, partner), device_id_type=MESH)
    pl.semaphore_signal(barrier, inc=1, device_id=(rep, across), device_id_type=MESH)

    @pl.when(z < 3)
    def _():
        pl.semaphore_signal(barrier, inc=1, device_id=(rep, me + 2), device_id_type=MESH)

    @pl.when(z > 0)
    def _():
        pl.semaphore_signal(barrier, inc=1, device_id=(rep, me - 2), device_id_type=MESH)

    @pl.when(mid)
    def _():
        pl.semaphore_wait(barrier, 4)

    @pl.when(corner)
    def _():
        pl.semaphore_wait(barrier, 3)

    def turn(i, carry):
        for sub in range(3):
            for name in ORDER:
                for kind in ("y", "z"):
                    lag = LAGS[kind].get(name)
                    if lag is None:
                        continue
                    x = weights[(sub - lag) % 3]
                    r = i + (sub - lag) // 3
                    ok = (r >= 0) & (r < ROUNDS)
                    some, is_z = kinds(x.which, r, name in GATHER)
                    if name in ("fetch", "moments"):
                        if kind == "z":
                            continue
                    elif kind not in some:
                        continue
                    elif is_z is not None:
                        ok = ok & (is_z if kind == "z" else jnp.logical_not(is_z))
                    pl.when(ok)(functools.partial(stages[name], x, kind, r))
        return carry

    longest = max(max(kind.values()) for kind in LAGS.values())
    lax.fori_loop(0, ROUNDS + (longest + 2) // 3, turn, 0)

    for x in weights:
        for slot in range(SLOTS):
            left(x.s.at[slot, pl.ds(0, 7)], x.ss.at[slot])
        def gathered(r, carry):
            some, is_z = kinds(x.which, r, True)
            for kind in some:

                def sent():
                    left(x.s.at[0, pl.ds(0, 4 if kind == "y" else 1)], x.ay.at[r])
                    pl.when(mid)(lambda: left(x.s.at[pl.ds(0, 1 if kind == "y" else 2), pl.ds(0, 5)], x.az.at[r]))
                    pl.when(corner)(lambda: left(x.s.at[0, pl.ds(0, 1 if kind == "y" else 2)], x.az.at[r]))

                pl.when(True if is_z is None else is_z if kind == "z" else jnp.logical_not(is_z))(sent)
            return carry

        lax.fori_loop(0, ROUNDS, gathered, 0)
        left(x.out.at[:, :, 0], x.ds)
        left(x.out.at[:, :, 0], x.ad)
        arrive(x.out.at[:, :, 0], x.adr)
        if not HELD[x.which]:
            arrive(x.wb, x.lo)
        for r in range(ROUNDS - LOADS, ROUNDS):
            for one in written(x, jnp.int32(r), r % LOADS):
                one.wait()


def finish(*refs):
    ins, outs, stages, ring = refs[:9], refs[9:18], refs[18:24], refs[24]
    sent, loaded, stored, taken, given = refs[25:]
    puts = []
    for i in range(2):
        rows = outs[i].shape[1] // 4
        for k in range(8):
            part = (k // 4, pl.ds(k % 4 * rows, rows))
            puts.append(pltpu.make_async_copy(ins[i].at[part], outs[i].at[part], sent.at[i, k]))
    loads = [pltpu.make_async_copy(ins[3 + i], stages[i], loaded.at[i]) for i in range(6)]
    stores = [pltpu.make_async_copy(stages[i], outs[3 + i], stored.at[i]) for i in range(6)]
    takes, gives = [], []
    rows = ring.shape[1]
    for k in range(2 * (3584 // rows)):
        part, slot = (k // (3584 // rows), pl.ds(k % (3584 // rows) * rows, rows)), k % RING
        takes.append(pltpu.make_async_copy(ins[2].at[part], ring.at[slot], taken.at[slot]))
        gives.append(pltpu.make_async_copy(ring.at[slot], outs[2].at[part], given.at[slot]))
    for one in (*takes[:RING], *loads, *puts):
        one.start()
    for k, (take, give) in enumerate(zip(takes, gives, strict=True)):
        take.wait()
        give.start()
        if k >= 1 and k - 1 + RING < len(takes):
            gives[k - 1].wait()
            takes[k - 1 + RING].start()
        if k % 2 and k // 2 < 6:
            loads[k // 2].wait()
            stores[k // 2].start()
    for one in (*gives[-RING:], *puts, *stores):
        one.wait()


def solution(mesh):
    def step(*arrays):
        terms, weights, m, v = (arrays[i : i + 3] for i in (0, 3, 6, 9))

        def cut(one):
            rows, cols = one.shape[-2:]
            return one.reshape(2, 8, 2, rows // 16, cols)

        wide = [cut(one) for one in weights]
        outs = pl.pallas_call(
            kernel,
            out_shape=[*((pltpu.VMEM if held else jax.ShapeDtypeStruct)(one.shape, one.dtype) for held, one in zip(HELD, wide, strict=True)), *(pltpu.HBM(one.shape, one.dtype) for one in (*m, *v))],
            in_specs=[ANY] * 12,
            out_specs=[pl.BlockSpec(memory_space=pltpu.VMEM) if held else ANY for held in HELD] + [ANY] * 6,
            scratch_shapes=[one for i in range(3) for one in scratch(i)],
            compiler_params=pltpu.CompilerParams(collective_id=0, has_side_effects=True, vmem_limit_bytes=16 * 2**20),
            name="sum_step_gather",
        )(*(pltpu.with_memory_space_constraint(one, pltpu.HBM) for one in (*(cut(t[0]) for t in terms), *wide, *m, *v)))
        whole = [one.reshape(w.shape) for one, w in zip(outs[:3], weights, strict=True)]
        kept = [pltpu.with_memory_space_constraint(one, pltpu.HBM) for one in (whole[2], *outs[3:])]
        dma = pltpu.SemaphoreType.DMA
        return pl.pallas_call(
            finish,
            out_shape=[jax.ShapeDtypeStruct(one.shape, one.dtype) for one in (*whole[:2], *kept)],
            in_specs=[ANY] * 9,
            out_specs=[ANY] * 9,
            scratch_shapes=[*(pltpu.VMEM(one.shape, one.dtype) for one in kept[1:]), pltpu.VMEM((RING, 448, 1024), jnp.bfloat16), dma((2, 8)), dma((6,)), dma((6,)), dma((RING,)), dma((RING,))],
            compiler_params=pltpu.CompilerParams(vmem_limit_bytes=16 * 2**20),
            name="finish",
        )(*whole[:2], *kept)

    all_of, cut = P(None, None, None), P(None, "dp", None)
    return jax.shard_map(
        step,
        mesh=mesh,
        in_specs=(P(("rep", "dp"), None, None, None),) * 3 + (all_of,) * 3 + (cut,) * 6,
        out_specs=(P("rep", None, None),) * 3 + (P("rep", "dp", None),) * 6,
        check_vma=False,
    )
```
